32 devices in a mesh: rp: 8 (over y, x, core), re: 4 (over z).
Axes of the slice: x: 2, y: 2, z: 4, core: 2. Of those that a mesh axis runs over, the one named last changes fastest.
Arguments:
- coupling: bfloat16 [128, 4, 2, 6, 4096], P('rp', 're'), may hold values from -1.25 to 1.25
- rp_coords: int32 [3, 128], P(None, 'rp'), may hold values from -8 to 8
- degeneracy: int32 [128], P('rp'), may hold values from 1 to 8
- qpoints: int32 [3, 64], replicated, may hold values from 0 to 15
- eigvec: float32 [64, 2, 6, 6], P('rp'), may hold values from -1.75 to 1.75
Outputs:
- coupling_q: float32 [64, 4, 2, 6, 4096], P('rp', None, None, None, 're')
The draws below stay inside these ranges and needn't reach their ends.
All inputs are finite; a program needn't handle non-finite values.
Results may differ from the reference program's by a relative error of at most 0.0042.
Values may be sent and summed in bfloat16 or wider, within the bound.
A program may use at most 64 MiB of HBM per device.

```python
import math
import jax
import jax.numpy as jnp
from jax import lax

NW = 64
MODES = 6
QGRID = 16
RMAX = 8
RP = 128
RE = 4
Q = 64


def plant(drawn, stream_key, smallest, top_value):
    longest = drawn.shape.index(max(drawn.shape))
    spots = []
    for shift in (0, 1):
        where = [jax.random.randint(jax.random.fold_in(stream_key, axis), (), 0, length) for axis, length in enumerate(drawn.shape)]
        where[longest] = (where[longest] + shift) % drawn.shape[longest]
        spots.append(tuple(where))
    return drawn.at[spots[0]].set(smallest).at[spots[1]].set(top_value)


def shard_levels(own_key, dims, pieces, low, top_value):
    gain = 1.0
    for dim, shards_of in pieces:
        steps = jax.random.uniform(jax.random.fold_in(jax.random.fold_in(own_key, 6), dim), (shards_of,), jnp.float32, low / len(pieces), top_value / len(pieces))
        gain = gain * jnp.repeat(jnp.exp(steps), dims[dim] // shards_of).reshape((-1,) + (1,) * (len(dims) - 1 - dim))
    return gain


def centred(rng, extent, width, bound, shards=(), dtype=jnp.bfloat16):
    result = width * jax.random.normal(rng, extent, jnp.float32)
    if shards:
        result = result * shard_levels(rng, extent, shards, -0.22, 0.18)
    return jnp.clip(result, -bound, bound).astype(dtype)


def setup_inputs(seed: int = 0) -> dict:
    streams_of = jax.random.split(jax.random.key(seed), 6)
    return {
        "coupling": centred(streams_of[0], (RP, RE, 2, MODES, NW * NW), (RP // 5) ** -0.5, 1.25, ((0, 8), (1, 4))),
        "rp_coords": plant(jax.random.randint(streams_of[1], (3, RP), 0 - RMAX, RMAX + 1), jax.random.fold_in(streams_of[1], 1), 0 - RMAX, RMAX).astype(jnp.int32),
        "degeneracy": plant(jax.random.randint(streams_of[2], (RP,), 1, 9), jax.random.fold_in(streams_of[2], 1), 1, 8).astype(jnp.int32),
        "qpoints": plant(jax.random.randint(streams_of[3], (3, Q), 0, QGRID), jax.random.fold_in(streams_of[3], 1), 0, QGRID - 1).astype(jnp.int32),
        "eigvec": centred(streams_of[4], (Q, 2, MODES, MODES), (2 * MODES) ** -0.5, 1.75, ((0, 8),), jnp.float32),
    }


def phases(points, coords, degeneracy):
    turns = jnp.mod(points[0][:, None] * coords[0][None, :], QGRID)
    turns = turns + jnp.mod(points[1][:, None] * coords[1][None, :], QGRID)
    turns = turns + jnp.mod(points[2][:, None] * coords[2][None, :], QGRID)
    turns = jnp.mod(turns, QGRID)
    angles = turns.astype(jnp.float32) * (2.0 * math.pi / QGRID)
    weights = 1.0 / degeneracy.astype(jnp.float32)
    table = jnp.concatenate([jnp.cos(angles) * weights[None, :], jnp.sin(angles) * weights[None, :]], axis=0)
    return table.astype(jnp.bfloat16)


def combine(table, coupling):
    point_count = table.shape[0] // 2
    product = jnp.dot(table, coupling.reshape(coupling.shape[0], -1), preferred_element_type=jnp.float32)
    product = product.reshape((2, point_count) + coupling.shape[1:])
    real_part = product[0, :, :, 0] - product[1, :, :, 1]
    imag_part = product[0, :, :, 1] + product[1, :, :, 0]
    return jnp.stack([real_part, imag_part], axis=2)


def mode_mix(values, matrix):
    return jnp.einsum("qrkp,qkn->qrnp", values, matrix, precision=lax.Precision.HIGHEST)


def rotate(summed, eigvec):
    real_in = summed[:, :, 0]
    imag_in = summed[:, :, 1]
    vec_real = eigvec[:, 0]
    vec_imag = eigvec[:, 1]
    real_out = mode_mix(real_in, vec_real) - mode_mix(imag_in, vec_imag)
    imag_out = mode_mix(real_in, vec_imag) + mode_mix(imag_in, vec_real)
    return jnp.stack([real_out, imag_out], axis=2)


def reference(coupling, rp_coords, degeneracy, qpoints, eigvec):
    table = phases(qpoints, rp_coords, degeneracy)
    summed = combine(table, coupling)
    return rotate(summed, eigvec)
```

```python
import functools
import math

import jax
import jax.numpy as jnp
from jax import lax
from jax.experimental import pallas as pl
from jax.experimental.pallas import tpu as pltpu
from jax.sharding import PartitionSpec as P

QGRID = 16
MESH = pl.DeviceIdType.MESH


def phases(points, coords, degeneracy):
    turns = jnp.mod(points[0][:, None] * coords[0][None, :], QGRID)
    turns = turns + jnp.mod(points[1][:, None] * coords[1][None, :], QGRID)
    turns = turns + jnp.mod(points[2][:, None] * coords[2][None, :], QGRID)
    turns = jnp.mod(turns, QGRID)
    angles = turns.astype(jnp.float32) * (2.0 * math.pi / QGRID)
    weights = 1.0 / degeneracy.astype(jnp.float32)
    table = jnp.concatenate(
        [jnp.cos(angles) * weights[None, :], jnp.sin(angles) * weights[None, :]], axis=0
    )
    return table.astype(jnp.bfloat16)


def combine(table, coupling):
    point_count = table.shape[0] // 2
    product = jnp.dot(
        table, coupling.reshape(coupling.shape[0], -1), preferred_element_type=jnp.float32
    )
    product = product.reshape((2, point_count) + coupling.shape[1:])
    real_part = product[0, :, :, 0] - product[1, :, :, 1]
    imag_part = product[0, :, :, 1] + product[1, :, :, 0]
    return jnp.stack([real_part, imag_part], axis=2)


def mode_mix(values, matrix):
    return jnp.einsum("qrkp,qkn->qrnp", values, matrix, precision=lax.Precision.HIGHEST)


def rotate(summed, eigvec):
    real_in = summed[:, :, 0]
    imag_in = summed[:, :, 1]
    vec_real = eigvec[:, 0]
    vec_imag = eigvec[:, 1]
    real_out = mode_mix(real_in, vec_real) - mode_mix(imag_in, vec_imag)
    imag_out = mode_mix(real_in, vec_imag) + mode_mix(imag_in, vec_real)
    return jnp.stack([real_out, imag_out], axis=2)


def to_owners(all_points):
    return lax.all_to_all(all_points, "rp", split_axis=0, concat_axis=3, tiled=True)


def per_device(coupling, rp_coords, degeneracy, qpoints, eigvec):
    stacked = jnp.concatenate([rp_coords, degeneracy[None, :]], axis=0)
    lattice = lax.all_gather(stacked, "rp", axis=1, tiled=True)
    table = phases(qpoints, lattice[:3], lattice[3])
    rp_count = lax.axis_size("rp")
    re_count = lax.axis_size("re")
    local_rp, local_re, parts, mode_count, pair_count = coupling.shape
    q_local = eigvec.shape[0]
    pair_share = pair_count // re_count
    block_cols = mode_count * pair_share
    inner = block_cols // rp_count
    reordered = coupling.reshape(local_rp, local_re, parts, mode_count, re_count, pair_share)
    reordered = jnp.swapaxes(reordered, 3, 4)
    reordered = reordered.reshape(local_rp, local_re, parts, re_count, rp_count, inner)
    reordered = jnp.swapaxes(reordered, 3, 4)
    reordered = reordered.reshape(local_rp, local_re, parts, rp_count * re_count * inner)
    moved = lax.all_to_all(
        lax.all_to_all(reordered, "rp", split_axis=3, concat_axis=0, tiled=True),
        "re",
        split_axis=3,
        concat_axis=1,
        tiled=True,
    )
    all_points = combine(table, moved)
    summed = to_owners(all_points)
    summed = summed.reshape(q_local, summed.shape[1], parts, mode_count, pair_share)
    return rotate(summed, eigvec)


def column_of(angle):
    return [math.cos(2.0 * math.pi * (step - angle) / QGRID) for step in range(QGRID)]


def pick(turns, values):
    picked = jnp.full(turns.shape, values[0], jnp.float32)
    for step in range(1, QGRID):
        picked = jnp.where(turns == step, jnp.float32(values[step]), picked)
    return picked


def flip(index, bits):
    for bit in (1, 2, 4):
        if bits & bit:
            index = index + bit - 2 * bit * (index // bit % 2)
    return index


def place(index, gather):
    return 2 * (index // gather % 2) + index % 2


def rotation_kernel(
    n,
    planes,
    coupling,
    coords,
    degeneracy,
    eigvec,
    points,
    out,
    gathered,
    all_coords,
    all_degeneracy,
    all_eigvec,
    table_rows,
    vectors,
    kept,
    leaving,
    arriving,
    turned,
    own_sem,
    small_send,
    small_recv,
    first_send,
    first_recv,
    middle_send,
    middle_recv,
    last_send,
    last_recv,
):
    me = lax.axis_index("rp")
    plane = lax.axis_index("re")
    local_rp, modes, parts, pairs = coupling.shape
    lanes = gathered.shape[-1]
    q_local = eigvec.shape[-1]
    group = 4
    tile = parts * q_local
    half = group * tile
    width = group * local_rp * parts
    steps = (2, 3, 1, 0)
    sets = ((0, 4, 2), (1, 2, 4))
    near = (0, 1, 4, 5, 2, 3)

    barrier = pltpu.get_barrier_semaphore()

    def greet(bits, step):
        pl.semaphore_signal(
            barrier,
            inc=1,
            device_id={"rp": flip(me, bits), "re": flip(plane, step)},
            device_id_type=MESH,
        )

    for step in steps:
        for bits in near:
            if bits or step:
                greet(bits, step)
    pl.semaphore_wait(barrier, len(near) * planes - 1)

    def local(source, target, index):
        return pltpu.make_async_copy(source, target, own_sem.at[index])

    def remote(source, target, send, recv, bits, step=0):
        return pltpu.make_async_remote_copy(
            src_ref=source,
            dst_ref=target,
            send_sem=send,
            recv_sem=recv,
            device_id={"rp": flip(me, bits), "re": flip(plane, step)},
            device_id_type=MESH,
        )

    def members(gather):
        return (gather + 1, gather, 1)

    def small_copies(sender):
        copies = []
        for index, gather, _ in sets:
            for turn, bits in enumerate(members(gather)):
                slot = place(me if sender else flip(me, bits), gather)
                at = index * 3 + turn
                for kind, (held, full) in enumerate(
                    ((coords, all_coords), (degeneracy, all_degeneracy))
                ):
                    copies.append(
                        remote(
                            held,
                            full.at[index, slot],
                            small_send.at[kind, at],
                            small_recv.at[kind, at],
                            bits,
                        )
                    )
        for turn, bits in enumerate(near):
            if bits:
                copies.append(
                    remote(
                        eigvec,
                        all_eigvec.at[turn],
                        small_send.at[2, turn],
                        small_recv.at[2, turn],
                        bits,
                    )
                )
        return copies

    def small_own():
        copies = []
        for index, gather, _ in sets:
            slot = place(me, gather)
            copies.append(local(coords, all_coords.at[index, slot], 2 * index))
            copies.append(local(degeneracy, all_degeneracy.at[index, slot], 2 * index + 1))
        copies.append(local(eigvec, all_eigvec.at[0], 4))
        return copies

    def piece(step, index, owner, gather):
        block = (flip(plane, step) * 2 + index) * group + place(owner, gather)
        return coupling.at[:, :, :, pl.ds(pl.multiple_of(block * lanes, lanes), lanes)]

    def landing(step, index, origin, gather):
        return gathered.at[step, index, pl.ds(place(origin, gather) * local_rp, local_rp)]

    def first_copy(step, index, gather, turn, bits, sender):
        origin = me if sender else flip(me, bits)
        return remote(
            piece(step, index, flip(me, bits), gather),
            landing(step, index, origin, gather),
            first_send.at[step, index, turn],
            first_recv.at[step, index, turn],
            bits,
        )

    def first_own(step, index, gather):
        return local(
            piece(step, index, me, gather),
            landing(step, index, me, gather),
            5 + 2 * step + index,
        )

    def send_first(step):
        for turn in range(3):
            for index, gather, _ in sets:
                first_copy(step, index, gather, turn, members(gather)[turn], True).start()
        for index, gather, _ in sets:
            first_own(step, index, gather).start()

    def middle_copy(step, index, other):
        return remote(
            leaving.at[step, index],
            arriving.at[step, index],
            middle_send.at[step, index],
            middle_recv.at[step, index],
            other,
        )

    def final_block(index, origin, gather):
        return index * group + place(origin, gather)

    def last_copy(step, index, gather, turn, bits, sender):
        origin = me if sender else flip(me, bits)
        home = plane if sender else flip(plane, step)
        source = turned.at[step, index, turn]
        target = out.at[home, final_block(index, origin, gather)]
        if not bits and not step:
            return local(source, target, 13 + index)
        return remote(
            source,
            target,
            last_send.at[step, index, turn],
            last_recv.at[step, index, turn],
            bits,
            step,
        )

    for copy in small_copies(True) + small_own():
        copy.start()
    for step in steps[:2]:
        send_first(step)
    for copy in small_own():
        copy.wait()
    for copy in small_copies(False):
        copy.wait_recv()

    columns = lax.broadcasted_iota(jnp.int32, (group * local_rp, width), 1)
    repeat = columns // parts == lax.broadcasted_iota(jnp.int32, (group * local_rp, width), 0)
    repeat = repeat.astype(jnp.bfloat16)

    def twice(full, index):
        row = jnp.concatenate([full[index, slot] for slot in range(group)], axis=1)
        row = row.astype(jnp.float32).astype(jnp.bfloat16)
        return jnp.dot(row, repeat, preferred_element_type=jnp.float32)

    q_count = n * q_local
    real_part = lax.broadcasted_iota(jnp.int32, (q_count, width), 1) % parts == 0
    tables = []
    for index, gather, other in sets:
        turns = lax.dot_general(
            points[...].astype(jnp.float32).astype(jnp.bfloat16),
            twice(all_coords, index).astype(jnp.bfloat16),
            (((0,), (0,)), ((), ())),
            preferred_element_type=jnp.float32,
        )
        turns = turns.astype(jnp.int32) & (QGRID - 1)
        weights = 1.0 / twice(all_degeneracy, index)
        cos = pick(turns, column_of(0.0)) * weights
        sin = pick(turns, column_of(QGRID / 4)) * weights
        to_real = jnp.where(real_part, cos, -sin)
        to_imag = jnp.where(real_part, sin, cos)
        mine = me // other % 2
        for owner in range(n):
            side = owner // other % 2
            apart = side + mine - 2 * side * mine
            row = pl.multiple_of((1 - apart) * half + place(owner, gather) * tile, tile)
            rows = slice(owner * q_local, (owner + 1) * q_local)
            table_rows[index, pl.ds(row, q_local), :] = to_real[rows]
            table_rows[index, pl.ds(row + q_local, q_local), :] = to_imag[rows]

    for turn in range(len(near)):
        flat = all_eigvec[turn].reshape(modes * modes * parts, q_local).T
        for entry in range(modes * modes * parts):
            vectors[turn, entry] = jnp.broadcast_to(flat[:, entry : entry + 1], (q_local, lanes))

    def gather_step(step):
        for index, gather, other in sets:
            first_own(step, index, gather).wait()
            for turn, bits in enumerate(members(gather)):
                first_copy(step, index, gather, turn, bits, False).wait_recv()
            table = table_rows[index].astype(jnp.bfloat16)
            for mode in range(modes):
                product = jnp.dot(
                    table,
                    gathered[step, index, :, mode].reshape(width, lanes),
                    preferred_element_type=jnp.float32,
                )
                at = slice(mode * lanes, (mode + 1) * lanes)
                leaving[step, index, :, at] = product[:half].astype(jnp.bfloat16)
                kept[step, index, :, at] = product[half:]
            middle_copy(step, index, other).start()

    def rotate_step(step):
        for index, gather, other in sets:
            middle_copy(step, index, other).wait_recv()
            for turn, bits in enumerate(members(gather) + (0,)):
                owner = near.index(bits)
                start = pl.multiple_of(place(flip(me, bits), gather) * tile, tile)
                rows = pl.ds(start, tile)
                real_in = []
                imag_in = []
                for k in range(modes):
                    at = slice(k * lanes, (k + 1) * lanes)
                    total = kept[step, index, rows, at] + arriving[
                        step, index, rows, at
                    ].astype(jnp.float32)
                    real_in.append(total[:q_local])
                    imag_in.append(total[q_local:])
                for mode in range(modes):
                    real_out = jnp.zeros((q_local, lanes), jnp.float32)
                    imag_out = jnp.zeros((q_local, lanes), jnp.float32)
                    for k in range(modes):
                        vec_real = vectors[owner, (k * modes + mode) * parts]
                        vec_imag = vectors[owner, (k * modes + mode) * parts + 1]
                        real_out += real_in[k] * vec_real - imag_in[k] * vec_imag
                        imag_out += real_in[k] * vec_imag + imag_in[k] * vec_real
                    turned[step, index, turn, mode] = jnp.concatenate(
                        [real_out, imag_out], axis=0
                    ).astype(jnp.bfloat16)
                last_copy(step, index, gather, turn, bits, True).start()

    gather_step(steps[0])
    send_first(steps[2])
    gather_step(steps[1])
    rotate_step(steps[0])
    send_first(steps[3])
    gather_step(steps[2])
    rotate_step(steps[1])
    gather_step(steps[3])
    rotate_step(steps[2])
    rotate_step(steps[3])

    for copy in small_copies(True):
        copy.wait_send()
    for step in steps:
        for index, gather, other in sets:
            for turn, bits in enumerate(members(gather)):
                first_copy(step, index, gather, turn, bits, True).wait_send()
            middle_copy(step, index, other).wait_send()
            for turn, bits in enumerate(members(gather) + (0,)):
                if bits or step:
                    last_copy(step, index, gather, turn, bits, True).wait_send()
                    last_copy(step, index, gather, turn, bits, False).wait_recv()
                else:
                    last_copy(step, index, gather, turn, bits, True).wait()


def spread_kernel(held, out, rows_of, sems):
    planes, blocks, modes, tile, lanes = held.shape
    q_local = tile // 2
    per_plane = modes * blocks * 2
    per_q = planes * per_plane

    def copies(source):
        return [
            pltpu.make_async_copy(
                rows_of.at[pl.ds(q * per_q + source * per_plane, per_plane)],
                out.at[pl.ds(q * per_q + source * per_plane, per_plane)],
                sems.at[source, q],
            )
            for q in range(q_local)
        ]

    for source in range(planes):
        for mode in range(modes):
            for block in range(blocks):
                values = held[source, block, mode].astype(jnp.float32)
                row = source * per_plane + (mode * blocks + block) * 2
                rows_of[pl.ds(row, q_local, stride=per_q), :] = values[:q_local]
                rows_of[pl.ds(row + 1, q_local, stride=per_q), :] = values[q_local:]
        for copy in copies(source):
            copy.start()
    for source in range(planes):
        for copy in copies(source):
            copy.wait()


def exchanged(coupling, rp_coords, degeneracy, qpoints, eigvec):
    n = lax.axis_size("rp")
    planes = lax.axis_size("re")
    local_rp, local_re, parts, modes, pairs = coupling.shape
    q_local = eigvec.shape[0]
    lanes = pairs // planes // n
    group = n // 2
    tile = parts * q_local
    half = group * tile
    width = group * local_rp * parts
    entries = parts * modes * modes
    near = 6
    gathered = pl.pallas_call(
        functools.partial(rotation_kernel, n, planes),
        out_shape=jax.ShapeDtypeStruct((planes, n, modes, tile, lanes), jnp.bfloat16),
        in_specs=[
            pl.BlockSpec(memory_space=pltpu.HBM),
            pl.BlockSpec(memory_space=pltpu.HBM),
            pl.BlockSpec(memory_space=pltpu.HBM),
            pl.BlockSpec(memory_space=pltpu.HBM),
            pl.BlockSpec(memory_space=pltpu.VMEM),
        ],
        out_specs=pl.BlockSpec(memory_space=pl.ANY),
        scratch_shapes=[
            pltpu.VMEM((planes, 2, group * local_rp, modes, parts, lanes), jnp.bfloat16),
            pltpu.VMEM((2, group) + rp_coords.shape, jnp.int32),
            pltpu.VMEM((2, group, 1, local_rp), jnp.int32),
            pltpu.VMEM((near, modes * modes, parts, q_local), jnp.float32),
            pltpu.VMEM((2, 2 * half, width), jnp.float32),
            pltpu.VMEM((near, entries, q_local, lanes), jnp.float32),
            pltpu.VMEM((planes, 2, half, modes * lanes), jnp.float32),
            pltpu.VMEM((planes, 2, half, modes * lanes), jnp.bfloat16),
            pltpu.VMEM((planes, 2, half, modes * lanes), jnp.bfloat16),
            pltpu.VMEM((planes, 2, group, modes, tile, lanes), jnp.bfloat16),
            pltpu.SemaphoreType.DMA((15,)),
            pltpu.SemaphoreType.DMA((3, near)),
            pltpu.SemaphoreType.DMA((3, near)),
            pltpu.SemaphoreType.DMA((planes, 2, group - 1)),
            pltpu.SemaphoreType.DMA((planes, 2, group - 1)),
            pltpu.SemaphoreType.DMA((planes, 2)),
            pltpu.SemaphoreType.DMA((planes, 2)),
            pltpu.SemaphoreType.DMA((planes, 2, group)),
            pltpu.SemaphoreType.DMA((planes, 2, group)),
        ],
        compiler_params=pltpu.CompilerParams(
            collective_id=0, has_side_effects=True, vmem_limit_bytes=24 * 2**20
        ),
    )(
        jnp.swapaxes(coupling[:, 0], 1, 2),
        rp_coords,
        degeneracy[None, :],
        jnp.transpose(eigvec, (2, 3, 1, 0)).reshape(modes * modes, parts, q_local),
        qpoints,
    )
    rows = q_local * planes * modes * n * parts
    spread = pl.pallas_call(
        spread_kernel,
        out_shape=jax.ShapeDtypeStruct((rows, lanes), jnp.float32),
        in_specs=[pl.BlockSpec(memory_space=pltpu.VMEM)],
        out_specs=pl.BlockSpec(memory_space=pl.ANY),
        scratch_shapes=[
            pltpu.VMEM((rows, lanes), jnp.float32),
            pltpu.SemaphoreType.DMA((planes, q_local)),
        ],
        compiler_params=pltpu.CompilerParams(vmem_limit_bytes=24 * 2**20),
    )(gathered)
    spread = spread.reshape(q_local, planes, modes, n, parts, lanes)
    spread = jnp.transpose(spread, (0, 1, 4, 2, 3, 5))
    return spread.reshape(q_local, planes, parts, modes, n * lanes)


def fits(n, planes, coupling, eigvec):
    local_rp, local_re, parts, modes, pairs = coupling.shape
    return (
        local_re == 1
        and n == 8
        and planes == 4
        and local_rp * n == 128
        and parts * modes * modes <= 128
        and pairs // planes // n == 128
        and eigvec.shape[0] == 8
        and modes <= 8
    )


def either(coupling, rp_coords, degeneracy, qpoints, eigvec):
    if fits(lax.axis_size("rp"), lax.axis_size("re"), coupling, eigvec):
        return exchanged(coupling, rp_coords, degeneracy, qpoints, eigvec)
    return per_device(coupling, rp_coords, degeneracy, qpoints, eigvec)


def solution(mesh):
    return jax.shard_map(
        either,
        mesh=mesh,
        in_specs=(
            P("rp", "re", None, None, None),
            P(None, "rp"),
            P("rp"),
            P(),
            P("rp", None, None, None),
        ),
        out_specs=P("rp", None, None, None, "re"),
        check_vma=False,
    )
```

```python
import functools
import math

import jax
import jax.numpy as jnp
from jax import lax
from jax.experimental import pallas as pl
from jax.experimental.pallas import tpu as pltpu
from jax.sharding import PartitionSpec as P

QGRID = 16
MESH = pl.DeviceIdType.MESH


def phases(points, coords, degeneracy):
    turns = jnp.mod(points[0][:, None] * coords[0][None, :], QGRID)
    turns = turns + jnp.mod(points[1][:, None] * coords[1][None, :], QGRID)
    turns = turns + jnp.mod(points[2][:, None] * coords[2][None, :], QGRID)
    turns = jnp.mod(turns, QGRID)
    angles = turns.astype(jnp.float32) * (2.0 * math.pi / QGRID)
    weights = 1.0 / degeneracy.astype(jnp.float32)
    table = jnp.concatenate(
        [jnp.cos(angles) * weights[None, :], jnp.sin(angles) * weights[None, :]], axis=0
    )
    return table.astype(jnp.bfloat16)


def combine(table, coupling):
    point_count = table.shape[0] // 2
    product = jnp.dot(
        table, coupling.reshape(coupling.shape[0], -1), preferred_element_type=jnp.float32
    )
    product = product.reshape((2, point_count) + coupling.shape[1:])
    real_part = product[0, :, :, 0] - product[1, :, :, 1]
    imag_part = product[0, :, :, 1] + product[1, :, :, 0]
    return jnp.stack([real_part, imag_part], axis=2)


def mode_mix(values, matrix):
    return jnp.einsum("qrkp,qkn->qrnp", values, matrix, precision=lax.Precision.HIGHEST)


def rotate(summed, eigvec):
    real_in = summed[:, :, 0]
    imag_in = summed[:, :, 1]
    vec_real = eigvec[:, 0]
    vec_imag = eigvec[:, 1]
    real_out = mode_mix(real_in, vec_real) - mode_mix(imag_in, vec_imag)
    imag_out = mode_mix(real_in, vec_imag) + mode_mix(imag_in, vec_real)
    return jnp.stack([real_out, imag_out], axis=2)


def to_owners(all_points):
    return lax.all_to_all(all_points, "rp", split_axis=0, concat_axis=3, tiled=True)


def per_device(coupling, rp_coords, degeneracy, qpoints, eigvec):
    stacked = jnp.concatenate([rp_coords, degeneracy[None, :]], axis=0)
    lattice = lax.all_gather(stacked, "rp", axis=1, tiled=True)
    table = phases(qpoints, lattice[:3], lattice[3])
    rp_count = lax.axis_size("rp")
    re_count = lax.axis_size("re")
    local_rp, local_re, parts, mode_count, pair_count = coupling.shape
    q_local = eigvec.shape[0]
    pair_share = pair_count // re_count
    block_cols = mode_count * pair_share
    inner = block_cols // rp_count
    reordered = coupling.reshape(local_rp, local_re, parts, mode_count, re_count, pair_share)
    reordered = jnp.swapaxes(reordered, 3, 4)
    reordered = reordered.reshape(local_rp, local_re, parts, re_count, rp_count, inner)
    reordered = jnp.swapaxes(reordered, 3, 4)
    reordered = reordered.reshape(local_rp, local_re, parts, rp_count * re_count * inner)
    moved = lax.all_to_all(
        lax.all_to_all(reordered, "rp", split_axis=3, concat_axis=0, tiled=True),
        "re",
        split_axis=3,
        concat_axis=1,
        tiled=True,
    )
    all_points = combine(table, moved)
    summed = to_owners(all_points)
    summed = summed.reshape(q_local, summed.shape[1], parts, mode_count, pair_share)
    return rotate(summed, eigvec)


def column_of(angle):
    return [math.cos(2.0 * math.pi * (step - angle) / QGRID) for step in range(QGRID)]


def pick(turns, values):
    picked = jnp.full(turns.shape, values[0], jnp.float32)
    for step in range(1, QGRID):
        picked = jnp.where(turns == step, jnp.float32(values[step]), picked)
    return picked


def flip(index, bits):
    for bit in (1, 2, 4):
        if bits & bit:
            index = index + bit - 2 * bit * (index // bit % 2)
    return index


def place(index, gather):
    return 2 * (index // gather % 2) + index % 2


def rotation_kernel(
    n,
    planes,
    coupling,
    coords,
    degeneracy,
    eigvec,
    points_in,
    out,
    points,
    gathered,
    all_coords,
    all_degeneracy,
    all_eigvec,
    table_rows,
    vectors,
    kept,
    leaving,
    arriving,
    turned,
    own_sem,
    small_send,
    small_recv,
    first_send,
    first_recv,
    middle_send,
    middle_recv,
    last_send,
    last_recv,
    above_sem,
):
    me = lax.axis_index("rp")
    plane = lax.axis_index("re")
    local_rp, modes, parts, pairs = coupling.shape
    lanes = gathered.shape[-1]
    q_local = eigvec.shape[-1]
    group = 4
    tile = parts * q_local
    half = group * tile
    width = group * local_rp * parts
    steps = (2, 3, 1, 0)
    sets = ((0, 4, 2), (1, 2, 4))
    near = (0, 1, 4, 5, 2, 3)

    barrier = pltpu.get_barrier_semaphore()

    def greet(semaphore, bits, level):
        pl.semaphore_signal(
            semaphore,
            inc=1,
            device_id={"rp": flip(me, bits), "re": level},
            device_id_type=MESH,
        )

    for bits in near[1:]:
        greet(barrier, bits, plane)
    for ahead in range(1, planes):

        @pl.when(plane + ahead < planes)
        def _():
            for bits in near:
                greet(barrier, bits, plane + ahead)

    pl.semaphore_wait(barrier, len(near) - 1 + len(near) * plane)
    for behind in range(1, planes):

        @pl.when(plane >= behind)
        def _():
            greet(above_sem, 0, plane - behind)

    def local(source, target, index):
        return pltpu.make_async_copy(source, target, own_sem.at[index])

    def remote(source, target, send, recv, bits, step=0):
        return pltpu.make_async_remote_copy(
            src_ref=source,
            dst_ref=target,
            send_sem=send,
            recv_sem=recv,
            device_id={"rp": flip(me, bits), "re": flip(plane, step)},
            device_id_type=MESH,
        )

    def members(gather):
        return (gather + 1, gather, 1)

    def small_copies(sender):
        copies = []
        for index, gather, _ in sets:
            for turn, bits in enumerate(members(gather)):
                slot = place(me if sender else flip(me, bits), gather)
                at = index * 3 + turn
                for kind, (held, full) in enumerate(
                    ((coords, all_coords), (degeneracy, all_degeneracy))
                ):
                    copies.append(
                        remote(
                            held,
                            full.at[index, slot],
                            small_send.at[kind, at],
                            small_recv.at[kind, at],
                            bits,
                        )
                    )
        for turn, bits in enumerate(near):
            if bits:
                copies.append(
                    remote(
                        eigvec,
                        all_eigvec.at[turn],
                        small_send.at[2, turn],
                        small_recv.at[2, turn],
                        bits,
                    )
                )
        return copies

    def small_own():
        copies = []
        for index, gather, _ in sets:
            slot = place(me, gather)
            copies.append(local(coords, all_coords.at[index, slot], 2 * index))
            copies.append(local(degeneracy, all_degeneracy.at[index, slot], 2 * index + 1))
        copies.append(local(eigvec, all_eigvec.at[0], 4))
        copies.append(local(points_in, points, 15))
        return copies

    def piece(step, index, owner, gather):
        block = (flip(plane, step) * 2 + index) * group + place(owner, gather)
        return coupling.at[:, :, :, pl.ds(pl.multiple_of(block * lanes, lanes), lanes)]

    def landing(step, index, origin, gather):
        return gathered.at[step, index, pl.ds(place(origin, gather) * local_rp, local_rp)]

    def first_copy(step, index, gather, turn, bits, sender):
        origin = me if sender else flip(me, bits)
        return remote(
            piece(step, index, flip(me, bits), gather),
            landing(step, index, origin, gather),
            first_send.at[step, index, turn],
            first_recv.at[step, index, turn],
            bits,
        )

    def first_own(step, index, gather):
        return local(
            piece(step, index, me, gather),
            landing(step, index, me, gather),
            5 + 2 * step + index,
        )

    def send_first(step):
        for turn in range(3):
            for index, gather, _ in sets:
                first_copy(step, index, gather, turn, members(gather)[turn], True).start()
        for index, gather, _ in sets:
            first_own(step, index, gather).start()

    def middle_copy(step, index, other):
        return remote(
            leaving.at[step, index],
            arriving.at[step, index],
            middle_send.at[step, index],
            middle_recv.at[step, index],
            other,
        )

    def final_block(index, origin, gather):
        return index * group + place(origin, gather)

    def last_copy(step, index, gather, turn, bits, sender):
        origin = me if sender else flip(me, bits)
        home = plane if sender else flip(plane, step)
        source = turned.at[step, index, turn]
        target = out.at[home, final_block(index, origin, gather)]
        if not bits and not step:
            return local(source, target, 13 + index)
        return remote(
            source,
            target,
            last_send.at[step, index, turn],
            last_recv.at[step, index, turn],
            bits,
            step,
        )

    for copy in small_copies(True) + small_own():
        copy.start()
    for step in steps[:2]:
        send_first(step)
    for copy in small_own():
        copy.wait()
    for copy in small_copies(False):
        copy.wait_recv()

    columns = lax.broadcasted_iota(jnp.int32, (group * local_rp, width), 1)
    repeat = columns // parts == lax.broadcasted_iota(jnp.int32, (group * local_rp, width), 0)
    repeat = repeat.astype(jnp.bfloat16)

    def twice(full, index):
        row = jnp.concatenate([full[index, slot] for slot in range(group)], axis=1)
        row = row.astype(jnp.float32).astype(jnp.bfloat16)
        return jnp.dot(row, repeat, preferred_element_type=jnp.float32)

    q_count = n * q_local
    real_part = lax.broadcasted_iota(jnp.int32, (q_count, width), 1) % parts == 0
    tables = []
    for index, gather, other in sets:
        turns = lax.dot_general(
            points[...].astype(jnp.float32).astype(jnp.bfloat16),
            twice(all_coords, index).astype(jnp.bfloat16),
            (((0,), (0,)), ((), ())),
            preferred_element_type=jnp.float32,
        )
        turns = turns.astype(jnp.int32) & (QGRID - 1)
        weights = 1.0 / twice(all_degeneracy, index)
        cos = pick(turns, column_of(0.0)) * weights
        sin = pick(turns, column_of(QGRID / 4)) * weights
        to_real = jnp.where(real_part, cos, -sin)
        to_imag = jnp.where(real_part, sin, cos)
        mine = me // other % 2
        for owner in range(n):
            side = owner // other % 2
            apart = side + mine - 2 * side * mine
            row = pl.multiple_of((1 - apart) * half + place(owner, gather) * tile, tile)
            rows = slice(owner * q_local, (owner + 1) * q_local)
            table_rows[index, pl.ds(row, q_local), :] = to_real[rows]
            table_rows[index, pl.ds(row + q_local, q_local), :] = to_imag[rows]

    for turn in range(len(near)):
        flat = all_eigvec[turn].reshape(modes * modes * parts, q_local).T
        for entry in range(modes * modes * parts):
            vectors[turn, entry] = jnp.broadcast_to(flat[:, entry : entry + 1], (q_local, lanes))

    def gather_step(step):
        for index, gather, other in sets:
            first_own(step, index, gather).wait()
            for turn, bits in enumerate(members(gather)):
                first_copy(step, index, gather, turn, bits, False).wait_recv()
            table = table_rows[index].astype(jnp.bfloat16)
            for mode in range(modes):
                product = jnp.dot(
                    table,
                    gathered[step, index, :, mode].reshape(width, lanes),
                    preferred_element_type=jnp.float32,
                )
                at = slice(mode * lanes, (mode + 1) * lanes)
                leaving[step, index, :, at] = product[:half].astype(jnp.bfloat16)
                kept[step, index, :, at] = product[half:]
            middle_copy(step, index, other).start()

    def rotate_step(step):
        for index, gather, other in sets:
            middle_copy(step, index, other).wait_recv()
            for turn, bits in enumerate(members(gather) + (0,)):
                owner = near.index(bits)
                start = pl.multiple_of(place(flip(me, bits), gather) * tile, tile)
                rows = pl.ds(start, tile)
                real_in = []
                imag_in = []
                for k in range(modes):
                    at = slice(k * lanes, (k + 1) * lanes)
                    total = kept[step, index, rows, at] + arriving[
                        step, index, rows, at
                    ].astype(jnp.float32)
                    real_in.append(total[:q_local])
                    imag_in.append(total[q_local:])
                for mode in range(modes):
                    real_out = jnp.zeros((q_local, lanes), jnp.float32)
                    imag_out = jnp.zeros((q_local, lanes), jnp.float32)
                    for k in range(modes):
                        vec_real = vectors[owner, (k * modes + mode) * parts]
                        vec_imag = vectors[owner, (k * modes + mode) * parts + 1]
                        real_out += real_in[k] * vec_real - imag_in[k] * vec_imag
                        imag_out += real_in[k] * vec_imag + imag_in[k] * vec_real
                    turned[step, index, turn, mode] = jnp.concatenate(
                        [real_out, imag_out], axis=0
                    ).astype(jnp.bfloat16)
                last_copy(step, index, gather, turn, bits, True).start()

    gather_step(steps[0])
    send_first(steps[2])
    gather_step(steps[1])

    @pl.when(plane < planes - 1)
    def _():
        pl.semaphore_wait(above_sem, planes - 1 - plane)

    rotate_step(steps[0])
    send_first(steps[3])
    gather_step(steps[2])
    rotate_step(steps[1])
    gather_step(steps[3])
    rotate_step(steps[2])
    rotate_step(steps[3])

    for copy in small_copies(True):
        copy.wait_send()
    for step in steps:
        for index, gather, other in sets:
            for turn, bits in enumerate(members(gather)):
                first_copy(step, index, gather, turn, bits, True).wait_send()
            middle_copy(step, index, other).wait_send()
            for turn, bits in enumerate(members(gather) + (0,)):
                if bits or step:
                    last_copy(step, index, gather, turn, bits, True).wait_send()
                    last_copy(step, index, gather, turn, bits, False).wait_recv()
                else:
                    last_copy(step, index, gather, turn, bits, True).wait()


def spread_kernel(held, out, rows_of, sems):
    planes, blocks, modes, tile, lanes = held.shape
    q_local = tile // 2
    per_plane = modes * blocks * 2
    per_q = planes * per_plane

    def copies(source):
        return [
            pltpu.make_async_copy(
                rows_of.at[pl.ds(q * per_q + source * per_plane, per_plane)],
                out.at[pl.ds(q * per_q + source * per_plane, per_plane)],
                sems.at[source, q],
            )
            for q in range(q_local)
        ]

    for source in range(planes):
        for mode in range(modes):
            for block in range(blocks):
                values = held[source, block, mode].astype(jnp.float32)
                row = source * per_plane + (mode * blocks + block) * 2
                rows_of[pl.ds(row, q_local, stride=per_q), :] = values[:q_local]
                rows_of[pl.ds(row + 1, q_local, stride=per_q), :] = values[q_local:]
        for copy in copies(source):
            copy.start()
    for source in range(planes):
        for copy in copies(source):
            copy.wait()


def in_hbm(value):
    return pltpu.with_memory_space_constraint(value, pltpu.HBM)


def exchanged(coupling, rp_coords, degeneracy, qpoints, eigvec):
    n = lax.axis_size("rp")
    planes = lax.axis_size("re")
    local_rp, local_re, parts, modes, pairs = coupling.shape
    q_local = eigvec.shape[0]
    lanes = pairs // planes // n
    group = n // 2
    tile = parts * q_local
    half = group * tile
    width = group * local_rp * parts
    entries = parts * modes * modes
    near = 6
    gathered = pl.pallas_call(
        functools.partial(rotation_kernel, n, planes),
        out_shape=jax.ShapeDtypeStruct((planes, n, modes, tile, lanes), jnp.bfloat16),
        in_specs=[
            pl.BlockSpec(memory_space=pltpu.HBM),
            pl.BlockSpec(memory_space=pltpu.HBM),
            pl.BlockSpec(memory_space=pltpu.HBM),
            pl.BlockSpec(memory_space=pltpu.HBM),
            pl.BlockSpec(memory_space=pltpu.HBM),
        ],
        out_specs=pl.BlockSpec(memory_space=pl.ANY),
        scratch_shapes=[
            pltpu.VMEM(qpoints.shape, jnp.int32),
            pltpu.VMEM((planes, 2, group * local_rp, modes, parts, lanes), jnp.bfloat16),
            pltpu.VMEM((2, group) + rp_coords.shape, jnp.int32),
            pltpu.VMEM((2, group, 1, local_rp), jnp.int32),
            pltpu.VMEM((near, modes * modes, parts, q_local), jnp.float32),
            pltpu.VMEM((2, 2 * half, width), jnp.float32),
            pltpu.VMEM((near, entries, q_local, lanes), jnp.float32),
            pltpu.VMEM((planes, 2, half, modes * lanes), jnp.float32),
            pltpu.VMEM((planes, 2, half, modes * lanes), jnp.bfloat16),
            pltpu.VMEM((planes, 2, half, modes * lanes), jnp.bfloat16),
            pltpu.VMEM((planes, 2, group, modes, tile, lanes), jnp.bfloat16),
            pltpu.SemaphoreType.DMA((16,)),
            pltpu.SemaphoreType.DMA((3, near)),
            pltpu.SemaphoreType.DMA((3, near)),
            pltpu.SemaphoreType.DMA((planes, 2, group - 1)),
            pltpu.SemaphoreType.DMA((planes, 2, group - 1)),
            pltpu.SemaphoreType.DMA((planes, 2)),
            pltpu.SemaphoreType.DMA((planes, 2)),
            pltpu.SemaphoreType.DMA((planes, 2, group)),
            pltpu.SemaphoreType.DMA((planes, 2, group)),
            pltpu.SemaphoreType.REGULAR,
        ],
        compiler_params=pltpu.CompilerParams(
            collective_id=0, has_side_effects=True, vmem_limit_bytes=24 * 2**20
        ),
    )(
        in_hbm(jnp.swapaxes(coupling[:, 0], 1, 2)),
        in_hbm(rp_coords),
        in_hbm(degeneracy[None, :]),
        in_hbm(jnp.transpose(eigvec, (2, 3, 1, 0)).reshape(modes * modes, parts, q_local)),
        in_hbm(qpoints),
    )
    rows = q_local * planes * modes * n * parts
    spread = pl.pallas_call(
        spread_kernel,
        out_shape=jax.ShapeDtypeStruct((rows, lanes), jnp.float32),
        in_specs=[pl.BlockSpec(memory_space=pltpu.VMEM)],
        out_specs=pl.BlockSpec(memory_space=pl.ANY),
        scratch_shapes=[
            pltpu.VMEM((rows, lanes), jnp.float32),
            pltpu.SemaphoreType.DMA((planes, q_local)),
        ],
        compiler_params=pltpu.CompilerParams(vmem_limit_bytes=24 * 2**20),
    )(gathered)
    spread = spread.reshape(q_local, planes, modes, n, parts, lanes)
    spread = jnp.transpose(spread, (0, 1, 4, 2, 3, 5))
    return spread.reshape(q_local, planes, parts, modes, n * lanes)


def fits(n, planes, coupling, eigvec):
    local_rp, local_re, parts, modes, pairs = coupling.shape
    return (
        local_re == 1
        and n == 8
        and planes == 4
        and local_rp * n == 128
        and parts * modes * modes <= 128
        and pairs // planes // n == 128
        and eigvec.shape[0] == 8
        and modes <= 8
    )


def either(coupling, rp_coords, degeneracy, qpoints, eigvec):
    if fits(lax.axis_size("rp"), lax.axis_size("re"), coupling, eigvec):
        return exchanged(coupling, rp_coords, degeneracy, qpoints, eigvec)
    return per_device(coupling, rp_coords, degeneracy, qpoints, eigvec)


def solution(mesh):
    return jax.shard_map(
        either,
        mesh=mesh,
        in_specs=(
            P("rp", "re", None, None, None),
            P(None, "rp"),
            P("rp"),
            P(),
            P("rp", None, None, None),
        ),
        out_specs=P("rp", None, None, None, "re"),
        check_vma=False,
    )
```

```python
import functools
import math

import jax
import jax.numpy as jnp
from jax import lax
from jax.experimental import pallas as pl
from jax.experimental.pallas import tpu as pltpu
from jax.sharding import PartitionSpec as P

QGRID = 16
MESH = pl.DeviceIdType.MESH


def phases(points, coords, degeneracy):
    turns = jnp.mod(points[0][:, None] * coords[0][None, :], QGRID)
    turns = turns + jnp.mod(points[1][:, None] * coords[1][None, :], QGRID)
    turns = turns + jnp.mod(points[2][:, None] * coords[2][None, :], QGRID)
    turns = jnp.mod(turns, QGRID)
    angles = turns.astype(jnp.float32) * (2.0 * math.pi / QGRID)
    weights = 1.0 / degeneracy.astype(jnp.float32)
    table = jnp.concatenate(
        [jnp.cos(angles) * weights[None, :], jnp.sin(angles) * weights[None, :]], axis=0
    )
    return table.astype(jnp.bfloat16)


def combine(table, coupling):
    point_count = table.shape[0] // 2
    product = jnp.dot(
        table, coupling.reshape(coupling.shape[0], -1), preferred_element_type=jnp.float32
    )
    product = product.reshape((2, point_count) + coupling.shape[1:])
    real_part = product[0, :, :, 0] - product[1, :, :, 1]
    imag_part = product[0, :, :, 1] + product[1, :, :, 0]
    return jnp.stack([real_part, imag_part], axis=2)


def mode_mix(values, matrix):
    return jnp.einsum("qrkp,qkn->qrnp", values, matrix, precision=lax.Precision.HIGHEST)


def rotate(summed, eigvec):
    real_in = summed[:, :, 0]
    imag_in = summed[:, :, 1]
    vec_real = eigvec[:, 0]
    vec_imag = eigvec[:, 1]
    real_out = mode_mix(real_in, vec_real) - mode_mix(imag_in, vec_imag)
    imag_out = mode_mix(real_in, vec_imag) + mode_mix(imag_in, vec_real)
    return jnp.stack([real_out, imag_out], axis=2)


def to_owners(all_points):
    return lax.all_to_all(all_points, "rp", split_axis=0, concat_axis=3, tiled=True)


def per_device(coupling, rp_coords, degeneracy, qpoints, eigvec):
    stacked = jnp.concatenate([rp_coords, degeneracy[None, :]], axis=0)
    lattice = lax.all_gather(stacked, "rp", axis=1, tiled=True)
    table = phases(qpoints, lattice[:3], lattice[3])
    rp_count = lax.axis_size("rp")
    re_count = lax.axis_size("re")
    local_rp, local_re, parts, mode_count, pair_count = coupling.shape
    q_local = eigvec.shape[0]
    pair_share = pair_count // re_count
    block_cols = mode_count * pair_share
    inner = block_cols // rp_count
    reordered = coupling.reshape(local_rp, local_re, parts, mode_count, re_count, pair_share)
    reordered = jnp.swapaxes(reordered, 3, 4)
    reordered = reordered.reshape(local_rp, local_re, parts, re_count, rp_count, inner)
    reordered = jnp.swapaxes(reordered, 3, 4)
    reordered = reordered.reshape(local_rp, local_re, parts, rp_count * re_count * inner)
    moved = lax.all_to_all(
        lax.all_to_all(reordered, "rp", split_axis=3, concat_axis=0, tiled=True),
        "re",
        split_axis=3,
        concat_axis=1,
        tiled=True,
    )
    all_points = combine(table, moved)
    summed = to_owners(all_points)
    summed = summed.reshape(q_local, summed.shape[1], parts, mode_count, pair_share)
    return rotate(summed, eigvec)


def column_of(angle):
    return [math.cos(2.0 * math.pi * (step - angle) / QGRID) for step in range(QGRID)]


def pick(turns, values):
    picked = jnp.full(turns.shape, values[0], jnp.float32)
    for step in range(1, QGRID):
        picked = jnp.where(turns == step, jnp.float32(values[step]), picked)
    return picked


def flip(index, bits):
    for bit in (1, 2, 4):
        if bits & bit:
            index = index + bit - 2 * bit * (index // bit % 2)
    return index


def place(index, gather):
    return 2 * (index // gather % 2) + index % 2


def rotation_kernel(
    n,
    planes,
    coupling,
    coords,
    degeneracy,
    eigvec,
    points_in,
    out,
    points,
    gathered,
    early,
    all_lattice,
    all_eigvec,
    table_rows,
    vectors,
    kept,
    leaving,
    arriving,
    turned,
    own_sem,
    small_send,
    small_recv,
    first_send,
    first_recv,
    middle_send,
    middle_recv,
    last_send,
    last_recv,
    above_sem,
):
    me = lax.axis_index("rp")
    plane = lax.axis_index("re")
    local_rp, modes, parts, pairs = coupling.shape
    share = pairs // planes
    lanes = gathered.shape[-1]
    q_local = eigvec.shape[-1]
    group = 4
    tile = parts * q_local
    half = group * tile
    pieces = 2
    width = group * local_rp * parts
    steps = (2, 3, 1, 0)
    sets = ((0, 4, 2), (1, 2, 4))
    near = (0, 1, 2, 3, 4, 5)

    barrier = pltpu.get_barrier_semaphore()

    def greet(semaphore, bits, level):
        pl.semaphore_signal(
            semaphore,
            inc=1,
            device_id={"rp": flip(me, bits), "re": level},
            device_id_type=MESH,
        )

    def local(source, target, index):
        return pltpu.make_async_copy(source, target, own_sem.at[index])

    def remote(source, target, send, recv, bits, step=0):
        return pltpu.make_async_remote_copy(
            src_ref=source,
            dst_ref=target,
            send_sem=send,
            recv_sem=recv,
            device_id={"rp": flip(me, bits), "re": flip(plane, step)},
            device_id_type=MESH,
        )

    def members(gather):
        return (gather + 1, gather, 1)

    def lattice_copies():
        return [
            remote(
                all_lattice.at[index, place(me, gather)],
                all_lattice.at[index, place(me, gather)],
                small_send.at[0],
                small_recv.at[0],
                bits,
            )
            for index, gather, _ in sets
            for turn, bits in enumerate(members(gather))
        ]

    def eigvec_copies():
        return [
            remote(
                all_eigvec.at[0],
                all_eigvec.at[turn],
                small_send.at[1],
                small_recv.at[1],
                bits,
            )
            for turn, bits in enumerate(near)
            if bits
        ]

    def bundle(held, send, recv):
        return remote(held, held, send, recv, 1)

    def lattice_all():
        held = all_lattice.at[:, pl.ds(0, group - 1)]
        return bundle(held, small_send.at[0], small_recv.at[0])

    def eigvec_all():
        return bundle(all_eigvec.at[pl.ds(1, len(near) - 1)], small_send.at[1], small_recv.at[1])

    def first_all(step, index):
        held = gathered.at[step, index, pl.ds(0, (group - 1) * local_rp)]
        return bundle(held, first_send.at[0], first_recv.at[step, index])

    def lattice_own():
        copies = []
        for index, gather, _ in sets:
            held = all_lattice.at[index, place(me, gather)]
            copies.append(local(coords, held.at[pl.ds(0, 3)], 2 * index))
            copies.append(local(degeneracy, held.at[pl.ds(3, 1)], 2 * index + 1))
        return copies

    def early_own():
        start = pl.multiple_of(flip(plane, steps[0]) * share, share)
        return local(coupling.at[:, :, :, pl.ds(start, share)], early, 16)

    eigvec_own = local(eigvec, all_eigvec.at[0], 4)
    points_own = local(points_in, points, 15)

    def piece(step, index, owner, gather):
        block = index * group + place(owner, gather)
        if step == steps[0]:
            return early.at[:, :, :, pl.ds(pl.multiple_of(block * lanes, lanes), lanes)]
        block = flip(plane, step) * 2 * group + block
        return coupling.at[:, :, :, pl.ds(pl.multiple_of(block * lanes, lanes), lanes)]

    def landing(step, index, gather):
        return gathered.at[step, index, pl.ds(place(me, gather) * local_rp, local_rp)]

    def first_copy(step, index, gather, bits):
        return remote(
            piece(step, index, flip(me, bits), gather),
            landing(step, index, gather),
            first_send.at[0],
            first_recv.at[step, index],
            bits,
        )

    def first_own(step, index, gather):
        return local(
            piece(step, index, me, gather),
            landing(step, index, gather),
            5 + 2 * step + index,
        )

    def send_first(step, turns=(0, 1, 2)):
        for turn in turns:
            for index, gather, _ in sets:
                first_copy(step, index, gather, members(gather)[turn]).start()
        if 2 in turns:
            for index, gather, _ in sets:
                first_own(step, index, gather).start()

    def middle_copy(step, index, other, side):
        rows = pl.ds(side * (half // pieces), half // pieces)
        return remote(
            leaving.at[step, index, rows],
            arriving.at[step, index, rows],
            middle_send.at[0],
            middle_recv.at[step, index, side],
            other,
        )

    def final_block(index, origin, gather):
        return index * group + place(origin, gather)

    def turned_at(step, index, side, core):
        return ((step * 2 + index) * 2 + side) * 2 + core

    def last_copy(step, index, gather, side, core):
        source = turned.at[turned_at(step, index, side, core)]
        target = out.at[plane * n + final_block(index, me, gather)]
        owner = flip(me, core) + gather * (side - me // gather % 2)
        return pltpu.make_async_remote_copy(
            src_ref=source,
            dst_ref=target,
            send_sem=last_send.at[0],
            recv_sem=last_recv.at[0],
            device_id={"rp": owner, "re": flip(plane, step)},
            device_id_type=MESH,
        )

    def last_all():
        count = n * planes - len(sets)
        return pltpu.make_async_remote_copy(
            src_ref=turned.at[pl.ds(0, count)],
            dst_ref=out.at[pl.ds(0, count)],
            send_sem=last_send.at[0],
            recv_sem=last_recv.at[0],
            device_id={"rp": flip(me, 1)},
            device_id_type=MESH,
        )

    def last_own(index, gather, side):
        return local(
            turned.at[turned_at(0, index, side, 0)],
            out.at[plane * n + final_block(index, me, gather)],
            13 + index,
        )

    def send_last(step, index, gather, side, core):
        if step or core:
            last_copy(step, index, gather, side, core).start()
            return
        same = me // gather % 2 == side

        @pl.when(same)
        def _():
            last_own(index, gather, side).start()

        @pl.when(jnp.logical_not(same))
        def _():
            last_copy(step, index, gather, side, core).start()

    early_own().start()
    for copy in lattice_own():
        copy.start()
    points_own.start()
    eigvec_own.start()
    for bits in near[1:]:
        greet(barrier, bits, plane)
    for ahead in range(1, planes):

        @pl.when(plane + ahead < planes)
        def _():
            for bits in near:
                greet(barrier, bits, plane + ahead)

    for copy in lattice_own():
        copy.wait()
    early_own().wait()
    pl.semaphore_wait(barrier, len(near) - 1 + len(near) * plane)
    for copy in lattice_copies():
        copy.start()
    send_first(steps[0])
    for behind in range(1, planes):

        @pl.when(plane >= behind)
        def _():
            greet(above_sem, 0, plane - behind)
    eigvec_own.wait()
    for copy in eigvec_copies():
        copy.start()
    send_first(steps[1])

    points_own.wait()
    lattice_all().wait_recv()

    columns = lax.broadcasted_iota(jnp.int32, (group * local_rp, width), 1)
    repeat = columns // parts == lax.broadcasted_iota(jnp.int32, (group * local_rp, width), 0)
    repeat = repeat.astype(jnp.bfloat16)

    def twice(index):
        row = jnp.concatenate([all_lattice[index, slot] for slot in range(group)], axis=1)
        row = row.astype(jnp.float32).astype(jnp.bfloat16)
        return jnp.dot(row, repeat, preferred_element_type=jnp.float32)

    q_count = n * q_local
    real_part = lax.broadcasted_iota(jnp.int32, (q_count, width), 1) % parts == 0
    tables = []
    for index, gather, other in sets:
        lattice = twice(index)
        turns = lax.dot_general(
            points[...].astype(jnp.float32).astype(jnp.bfloat16),
            lattice[:3].astype(jnp.bfloat16),
            (((0,), (0,)), ((), ())),
            preferred_element_type=jnp.float32,
        )
        turns = turns.astype(jnp.int32) & (QGRID - 1)
        weights = 1.0 / lattice[3:]
        cos = pick(turns, column_of(0.0)) * weights
        sin = pick(turns, column_of(QGRID / 4)) * weights
        to_real = jnp.where(real_part, cos, -sin)
        to_imag = jnp.where(real_part, sin, cos)
        mine = me // other % 2
        for owner in range(n):
            across = owner // other % 2
            apart = across + mine - 2 * across * mine
            row = pl.multiple_of((1 - apart) * half + place(owner, gather) * tile, tile)
            rows = slice(owner * q_local, (owner + 1) * q_local)
            table_rows[index, pl.ds(row, q_local), :] = to_real[rows]
            table_rows[index, pl.ds(row + q_local, q_local), :] = to_imag[rows]

    def gather_step(step):
        for index, gather, other in sets:
            first_own(step, index, gather).wait()
            first_all(step, index).wait_recv()
            table = table_rows[index].astype(jnp.bfloat16)
            for mode in range(modes):
                product = jnp.dot(
                    table,
                    gathered[step, index, :, mode].reshape(width, lanes),
                    preferred_element_type=jnp.float32,
                )
                at = slice(mode * lanes, (mode + 1) * lanes)
                leaving[step, index, :, at] = product[:half].astype(jnp.bfloat16)
                kept[step, index, :, at] = product[half:]
            for side in range(pieces):
                middle_copy(step, index, other, side).start()

    def rotate_step(step):
        for side in range(pieces):
            for index, gather, other in sets:
                middle_copy(step, index, other, side).wait_recv()
                apart = (me // gather + side) % 2
                for core in (1, 0):
                    start = pl.multiple_of((2 * side + (me + core) % 2) * tile, tile)
                    rows = pl.ds(start, tile)
                    owner = apart * gather + core
                    real_in = []
                    imag_in = []
                    for k in range(modes):
                        at = slice(k * lanes, (k + 1) * lanes)
                        total = kept[step, index, rows, at] + arriving[
                            step, index, rows, at
                        ].astype(jnp.float32)
                        real_in.append(total[:q_local])
                        imag_in.append(total[q_local:])
                    for mode in range(modes):
                        real_out = jnp.zeros((q_local, lanes), jnp.float32)
                        imag_out = jnp.zeros((q_local, lanes), jnp.float32)
                        for k in range(modes):
                            vec_real = vectors[owner, (k * modes + mode) * parts]
                            vec_imag = vectors[owner, (k * modes + mode) * parts + 1]
                            real_out += real_in[k] * vec_real - imag_in[k] * vec_imag
                            imag_out += real_in[k] * vec_imag + imag_in[k] * vec_real
                        turned[turned_at(step, index, side, core), mode] = jnp.concatenate(
                            [real_out, imag_out], axis=0
                        ).astype(jnp.bfloat16)
                    send_last(step, index, gather, side, core)

    gather_step(steps[0])
    eigvec_all().wait_recv()
    for turn in range(len(near)):
        flat = all_eigvec[turn].reshape(modes * modes * parts, q_local).T
        for entry in range(modes * modes * parts):
            vectors[turn, entry] = jnp.broadcast_to(flat[:, entry : entry + 1], (q_local, lanes))
    send_first(steps[2])
    gather_step(steps[1])

    @pl.when(plane < planes - 1)
    def _():
        pl.semaphore_wait(above_sem, planes - 1 - plane)

    rotate_step(steps[0])
    send_first(steps[3])
    gather_step(steps[2])
    rotate_step(steps[1])
    gather_step(steps[3])
    rotate_step(steps[2])
    rotate_step(steps[3])

    lattice_all().wait_send()
    eigvec_all().wait_send()
    everything = gathered.at[:, :, pl.ds(0, (group - 1) * local_rp)]
    bundle(everything, first_send.at[0], first_recv.at[0, 0]).wait_send()
    bundle(leaving, middle_send.at[0], middle_recv.at[0, 0, 0]).wait_send()
    for index, gather, _ in sets:
        last_own(index, gather, me // gather % 2).wait()
    last_all().wait_recv()
    last_all().wait_send()


def spread_kernel(planes, held, out, rows_of, sems):
    _, modes, tile, lanes = held.shape
    blocks = held.shape[0] // planes
    q_local = tile // 2
    per_plane = modes * blocks * 2
    per_q = planes * per_plane

    def copies(source):
        return [
            pltpu.make_async_copy(
                rows_of.at[pl.ds(q * per_q + source * per_plane, per_plane)],
                out.at[pl.ds(q * per_q + source * per_plane, per_plane)],
                sems.at[source, q],
            )
            for q in range(q_local)
        ]

    for source in range(planes):
        for mode in range(modes):
            for block in range(blocks):
                values = held[source * blocks + block, mode].astype(jnp.float32)
                row = source * per_plane + (mode * blocks + block) * 2
                rows_of[pl.ds(row, q_local, stride=per_q), :] = values[:q_local]
                rows_of[pl.ds(row + 1, q_local, stride=per_q), :] = values[q_local:]
        for copy in copies(source):
            copy.start()
    for source in range(planes):
        for copy in copies(source):
            copy.wait()


def in_hbm(value):
    return pltpu.with_memory_space_constraint(value, pltpu.HBM)


def exchanged(coupling, rp_coords, degeneracy, qpoints, eigvec):
    n = lax.axis_size("rp")
    planes = lax.axis_size("re")
    local_rp, local_re, parts, modes, pairs = coupling.shape
    q_local = eigvec.shape[0]
    lanes = pairs // planes // n
    group = n // 2
    tile = parts * q_local
    half = group * tile
    width = group * local_rp * parts
    entries = parts * modes * modes
    near = 6
    gathered = pl.pallas_call(
        functools.partial(rotation_kernel, n, planes),
        out_shape=jax.ShapeDtypeStruct((planes * n, modes, tile, lanes), jnp.bfloat16),
        in_specs=[
            pl.BlockSpec(memory_space=pltpu.HBM),
            pl.BlockSpec(memory_space=pltpu.HBM),
            pl.BlockSpec(memory_space=pltpu.HBM),
            pl.BlockSpec(memory_space=pltpu.HBM),
            pl.BlockSpec(memory_space=pltpu.HBM),
        ],
        out_specs=pl.BlockSpec(memory_space=pl.ANY),
        scratch_shapes=[
            pltpu.VMEM(qpoints.shape, jnp.int32),
            pltpu.VMEM((planes, 2, group * local_rp, modes, parts, lanes), jnp.bfloat16),
            pltpu.VMEM((local_rp, modes, parts, pairs // planes), jnp.bfloat16),
            pltpu.VMEM((2, group, rp_coords.shape[0] + 1, local_rp), jnp.int32),
            pltpu.VMEM((near, modes * modes, parts, q_local), jnp.float32),
            pltpu.VMEM((2, 2 * half, width), jnp.float32),
            pltpu.VMEM((near, entries, q_local, lanes), jnp.float32),
            pltpu.VMEM((planes, 2, half, modes * lanes), jnp.float32),
            pltpu.VMEM((planes, 2, half, modes * lanes), jnp.bfloat16),
            pltpu.VMEM((planes, 2, half, modes * lanes), jnp.bfloat16),
            pltpu.VMEM((planes * n, modes, tile, lanes), jnp.bfloat16),
            pltpu.SemaphoreType.DMA((17,)),
            pltpu.SemaphoreType.DMA((2,)),
            pltpu.SemaphoreType.DMA((2,)),
            pltpu.SemaphoreType.DMA((1,)),
            pltpu.SemaphoreType.DMA((planes, 2)),
            pltpu.SemaphoreType.DMA((1,)),
            pltpu.SemaphoreType.DMA((planes, 2, 2)),
            pltpu.SemaphoreType.DMA((1,)),
            pltpu.SemaphoreType.DMA((1,)),
            pltpu.SemaphoreType.REGULAR,
        ],
        compiler_params=pltpu.CompilerParams(
            collective_id=0, has_side_effects=True, vmem_limit_bytes=24 * 2**20
        ),
    )(
        in_hbm(jnp.swapaxes(coupling[:, 0], 1, 2)),
        in_hbm(rp_coords),
        in_hbm(degeneracy[None, :]),
        in_hbm(jnp.transpose(eigvec, (2, 3, 1, 0)).reshape(modes * modes, parts, q_local)),
        in_hbm(qpoints),
    )
    rows = q_local * planes * modes * n * parts
    spread = pl.pallas_call(
        functools.partial(spread_kernel, planes),
        out_shape=jax.ShapeDtypeStruct((rows, lanes), jnp.float32),
        in_specs=[pl.BlockSpec(memory_space=pltpu.VMEM)],
        out_specs=pl.BlockSpec(memory_space=pl.ANY),
        scratch_shapes=[
            pltpu.VMEM((rows, lanes), jnp.float32),
            pltpu.SemaphoreType.DMA((planes, q_local)),
        ],
        compiler_params=pltpu.CompilerParams(vmem_limit_bytes=24 * 2**20),
    )(gathered)
    spread = spread.reshape(q_local, planes, modes, n, parts, lanes)
    spread = jnp.transpose(spread, (0, 1, 4, 2, 3, 5))
    return spread.reshape(q_local, planes, parts, modes, n * lanes)


def fits(n, planes, coupling, eigvec):
    local_rp, local_re, parts, modes, pairs = coupling.shape
    return (
        local_re == 1
        and n == 8
        and planes == 4
        and local_rp * n == 128
        and parts * modes * modes <= 128
        and pairs // planes // n == 128
        and eigvec.shape[0] == 8
        and modes <= 8
    )


def either(coupling, rp_coords, degeneracy, qpoints, eigvec):
    if fits(lax.axis_size("rp"), lax.axis_size("re"), coupling, eigvec):
        return exchanged(coupling, rp_coords, degeneracy, qpoints, eigvec)
    return per_device(coupling, rp_coords, degeneracy, qpoints, eigvec)


def solution(mesh):
    return jax.shard_map(
        either,
        mesh=mesh,
        in_specs=(
            P("rp", "re", None, None, None),
            P(None, "rp"),
            P("rp"),
            P(),
            P("rp", None, None, None),
        ),
        out_specs=P("rp", None, None, None, "re"),
        check_vma=False,
    )
```

```python
import functools
import math

import jax
import jax.numpy as jnp
from jax import lax
from jax.experimental import pallas as pl
from jax.experimental.pallas import tpu as pltpu
from jax.sharding import PartitionSpec as P

QGRID = 16
MESH = pl.DeviceIdType.MESH


def phases(points, coords, degeneracy):
    turns = jnp.mod(points[0][:, None] * coords[0][None, :], QGRID)
    turns = turns + jnp.mod(points[1][:, None] * coords[1][None, :], QGRID)
    turns = turns + jnp.mod(points[2][:, None] * coords[2][None, :], QGRID)
    turns = jnp.mod(turns, QGRID)
    angles = turns.astype(jnp.float32) * (2.0 * math.pi / QGRID)
    weights = 1.0 / degeneracy.astype(jnp.float32)
    table = jnp.concatenate(
        [jnp.cos(angles) * weights[None, :], jnp.sin(angles) * weights[None, :]], axis=0
    )
    return table.astype(jnp.bfloat16)


def combine(table, coupling):
    point_count = table.shape[0] // 2
    product = jnp.dot(
        table, coupling.reshape(coupling.shape[0], -1), preferred_element_type=jnp.float32
    )
    product = product.reshape((2, point_count) + coupling.shape[1:])
    real_part = product[0, :, :, 0] - product[1, :, :, 1]
    imag_part = product[0, :, :, 1] + product[1, :, :, 0]
    return jnp.stack([real_part, imag_part], axis=2)


def mode_mix(values, matrix):
    return jnp.einsum("qrkp,qkn->qrnp", values, matrix, precision=lax.Precision.HIGHEST)


def rotate(summed, eigvec):
    real_in = summed[:, :, 0]
    imag_in = summed[:, :, 1]
    vec_real = eigvec[:, 0]
    vec_imag = eigvec[:, 1]
    real_out = mode_mix(real_in, vec_real) - mode_mix(imag_in, vec_imag)
    imag_out = mode_mix(real_in, vec_imag) + mode_mix(imag_in, vec_real)
    return jnp.stack([real_out, imag_out], axis=2)


def to_owners(all_points):
    return lax.all_to_all(all_points, "rp", split_axis=0, concat_axis=3, tiled=True)


def per_device(coupling, rp_coords, degeneracy, qpoints, eigvec):
    stacked = jnp.concatenate([rp_coords, degeneracy[None, :]], axis=0)
    lattice = lax.all_gather(stacked, "rp", axis=1, tiled=True)
    table = phases(qpoints, lattice[:3], lattice[3])
    rp_count = lax.axis_size("rp")
    re_count = lax.axis_size("re")
    local_rp, local_re, parts, mode_count, pair_count = coupling.shape
    q_local = eigvec.shape[0]
    pair_share = pair_count // re_count
    block_cols = mode_count * pair_share
    inner = block_cols // rp_count
    reordered = coupling.reshape(local_rp, local_re, parts, mode_count, re_count, pair_share)
    reordered = jnp.swapaxes(reordered, 3, 4)
    reordered = reordered.reshape(local_rp, local_re, parts, re_count, rp_count, inner)
    reordered = jnp.swapaxes(reordered, 3, 4)
    reordered = reordered.reshape(local_rp, local_re, parts, rp_count * re_count * inner)
    moved = lax.all_to_all(
        lax.all_to_all(reordered, "rp", split_axis=3, concat_axis=0, tiled=True),
        "re",
        split_axis=3,
        concat_axis=1,
        tiled=True,
    )
    all_points = combine(table, moved)
    summed = to_owners(all_points)
    summed = summed.reshape(q_local, summed.shape[1], parts, mode_count, pair_share)
    return rotate(summed, eigvec)


def column_of(angle):
    return [math.cos(2.0 * math.pi * (step - angle) / QGRID) for step in range(QGRID)]


def pick(turns, values):
    picked = jnp.full(turns.shape, values[0], jnp.float32)
    for step in range(1, QGRID):
        picked = jnp.where(turns == step, jnp.float32(values[step]), picked)
    return picked


def flip(index, bits):
    for bit in (1, 2, 4):
        if bits & bit:
            index = index + bit - 2 * bit * (index // bit % 2)
    return index


def place(index, gather):
    return 2 * (index // gather % 2) + index % 2


def rotation_kernel(
    n,
    planes,
    coupling,
    coords,
    degeneracy,
    eigvec,
    points_in,
    out,
    points,
    gathered,
    early,
    all_lattice,
    own_eigvec,
    all_eigvec,
    table_rows,
    vectors,
    kept,
    leaving,
    arriving,
    turned,
    own_sem,
    small_send,
    small_recv,
    first_send,
    first_recv,
    middle_send,
    middle_recv,
    last_send,
    last_recv,
    above_sem,
):
    me = lax.axis_index("rp")
    plane = lax.axis_index("re")
    local_rp, modes, parts, pairs = coupling.shape
    share = pairs // planes
    lanes = gathered.shape[-1]
    q_local = eigvec.shape[-1]
    group = 4
    tile = parts * q_local
    half = group * tile
    pieces = 2
    width = group * local_rp * parts
    steps = (2, 3, 1, 0)
    sets = ((0, 4, 2), (1, 2, 4))
    near = (0, 1, 2, 3, 4, 5)

    barrier = pltpu.get_barrier_semaphore()

    def greet(semaphore, bits, level):
        pl.semaphore_signal(
            semaphore,
            inc=1,
            device_id={"rp": flip(me, bits), "re": level},
            device_id_type=MESH,
        )

    def local(source, target, index):
        return pltpu.make_async_copy(source, target, own_sem.at[index])

    def remote(source, target, send, recv, bits, step=0):
        return pltpu.make_async_remote_copy(
            src_ref=source,
            dst_ref=target,
            send_sem=send,
            recv_sem=recv,
            device_id={"rp": flip(me, bits), "re": flip(plane, step)},
            device_id_type=MESH,
        )

    def members(gather):
        return (gather + 1, gather, 1)

    def lattice_copies():
        return [
            remote(
                all_lattice.at[index, place(me, gather)],
                all_lattice.at[index, place(me, gather)],
                small_send.at[0],
                small_recv.at[0],
                bits,
            )
            for index, gather, _ in sets
            for turn, bits in enumerate(members(gather))
        ]

    def eigvec_copies():
        return [
            remote(
                all_eigvec.at[0],
                all_eigvec.at[turn],
                small_send.at[1],
                small_recv.at[1],
                bits,
            )
            for turn, bits in enumerate(near)
            if bits
        ]

    def bundle(held, send, recv):
        return remote(held, held, send, recv, 1)

    def lattice_all():
        held = all_lattice.at[:, pl.ds(0, group - 1)]
        return bundle(held, small_send.at[0], small_recv.at[0])

    def eigvec_all():
        return bundle(all_eigvec.at[pl.ds(1, len(near) - 1)], small_send.at[1], small_recv.at[1])

    def first_all(step, index):
        held = gathered.at[step, index, pl.ds(0, (group - 1) * local_rp)]
        return bundle(held, first_send.at[0], first_recv.at[step, index])

    def lattice_own():
        copies = []
        for index, gather, _ in sets:
            held = all_lattice.at[index, place(me, gather)]
            copies.append(local(coords, held.at[pl.ds(0, 3)], 2 * index))
            copies.append(local(degeneracy, held.at[pl.ds(3, 1)], 2 * index + 1))
        return copies

    def early_own():
        start = pl.multiple_of(flip(plane, steps[0]) * share, share)
        return local(coupling.at[:, :, :, pl.ds(start, share)], early, 16)

    eigvec_own = local(eigvec, own_eigvec, 4)
    points_own = local(points_in, points, 15)

    def piece(step, index, owner, gather):
        block = index * group + place(owner, gather)
        if step == steps[0]:
            return early.at[:, :, :, pl.ds(pl.multiple_of(block * lanes, lanes), lanes)]
        block = flip(plane, step) * 2 * group + block
        return coupling.at[:, :, :, pl.ds(pl.multiple_of(block * lanes, lanes), lanes)]

    def landing(step, index, gather):
        return gathered.at[step, index, pl.ds(place(me, gather) * local_rp, local_rp)]

    def first_copy(step, index, gather, bits):
        return remote(
            piece(step, index, flip(me, bits), gather),
            landing(step, index, gather),
            first_send.at[0],
            first_recv.at[step, index],
            bits,
        )

    def first_own(step, index, gather):
        return local(
            piece(step, index, me, gather),
            landing(step, index, gather),
            5 + 2 * step + index,
        )

    def send_first(step, turns=(0, 1, 2)):
        for turn in turns:
            for index, gather, _ in sets:
                first_copy(step, index, gather, members(gather)[turn]).start()
        if 2 in turns:
            for index, gather, _ in sets:
                first_own(step, index, gather).start()

    def middle_copy(step, index, other, side):
        rows = pl.ds(side * (half // pieces), half // pieces)
        return remote(
            leaving.at[step, index, rows],
            arriving.at[step, index, rows],
            middle_send.at[0],
            middle_recv.at[step, index, side],
            other,
        )

    def final_block(index, origin, gather):
        return index * group + place(origin, gather)

    def turned_at(step, index, side, core):
        return ((step * 2 + index) * 2 + side) * 2 + core

    def last_copy(step, index, gather, side, core):
        source = turned.at[turned_at(step, index, side, core)]
        target = out.at[plane * n + final_block(index, me, gather)]
        owner = flip(me, core) + gather * (side - me // gather % 2)
        return pltpu.make_async_remote_copy(
            src_ref=source,
            dst_ref=target,
            send_sem=last_send.at[0],
            recv_sem=last_recv.at[0],
            device_id={"rp": owner, "re": flip(plane, step)},
            device_id_type=MESH,
        )

    def last_all():
        count = n * planes - len(sets)
        return pltpu.make_async_remote_copy(
            src_ref=turned.at[pl.ds(0, count)],
            dst_ref=out.at[pl.ds(0, count)],
            send_sem=last_send.at[0],
            recv_sem=last_recv.at[0],
            device_id={"rp": flip(me, 1)},
            device_id_type=MESH,
        )

    def last_own(index, gather, side):
        return local(
            turned.at[turned_at(0, index, side, 0)],
            out.at[plane * n + final_block(index, me, gather)],
            13 + index,
        )

    def send_last(step, index, gather, side, core):
        if step or core:
            last_copy(step, index, gather, side, core).start()
            return
        same = me // gather % 2 == side

        @pl.when(same)
        def _():
            last_own(index, gather, side).start()

        @pl.when(jnp.logical_not(same))
        def _():
            last_copy(step, index, gather, side, core).start()

    early_own().start()
    for copy in lattice_own():
        copy.start()
    points_own.start()
    eigvec_own.start()
    for bits in near[1:]:
        greet(barrier, bits, plane)
    for ahead in range(1, planes):

        @pl.when(plane + ahead < planes)
        def _():
            for bits in near:
                greet(barrier, bits, plane + ahead)

    for copy in lattice_own():
        copy.wait()
    early_own().wait()
    pl.semaphore_wait(barrier, len(near) - 1 + len(near) * plane)
    for copy in lattice_copies():
        copy.start()
    send_first(steps[0])
    for behind in range(1, planes):

        @pl.when(plane >= behind)
        def _():
            greet(above_sem, 0, plane - behind)
    eigvec_own.wait()
    entries = modes * modes * parts
    all_eigvec[0, :, :entries] = own_eigvec[...].reshape(entries, q_local).T
    for copy in eigvec_copies():
        copy.start()
    send_first(steps[1])

    points_own.wait()
    lattice_all().wait_recv()

    columns = lax.broadcasted_iota(jnp.int32, (group * local_rp, width), 1)
    repeat = columns // parts == lax.broadcasted_iota(jnp.int32, (group * local_rp, width), 0)
    repeat = repeat.astype(jnp.bfloat16)

    def twice(index):
        row = jnp.concatenate([all_lattice[index, slot] for slot in range(group)], axis=1)
        row = row.astype(jnp.float32).astype(jnp.bfloat16)
        return jnp.dot(row, repeat, preferred_element_type=jnp.float32)

    q_count = n * q_local
    real_part = lax.broadcasted_iota(jnp.int32, (q_count, width), 1) % parts == 0
    tables = []
    for index, gather, other in sets:
        lattice = twice(index)
        turns = lax.dot_general(
            points[...].astype(jnp.float32).astype(jnp.bfloat16),
            lattice[:3].astype(jnp.bfloat16),
            (((0,), (0,)), ((), ())),
            preferred_element_type=jnp.float32,
        )
        turns = turns.astype(jnp.int32) & (QGRID - 1)
        weights = 1.0 / lattice[3:]
        cos = pick(turns, column_of(0.0)) * weights
        sin = pick(turns, column_of(QGRID / 4)) * weights
        to_real = jnp.where(real_part, cos, -sin)
        to_imag = jnp.where(real_part, sin, cos)
        mine = me // other % 2
        for owner in range(n):
            across = owner // other % 2
            apart = across + mine - 2 * across * mine
            row = pl.multiple_of((1 - apart) * half + place(owner, gather) * tile, tile)
            rows = slice(owner * q_local, (owner + 1) * q_local)
            table_rows[index, pl.ds(row, q_local), :] = to_real[rows]
            table_rows[index, pl.ds(row + q_local, q_local), :] = to_imag[rows]

    def gather_step(step):
        for index, gather, other in sets:
            first_own(step, index, gather).wait()
            first_all(step, index).wait_recv()
            table = table_rows[index].astype(jnp.bfloat16)
            for mode in range(modes):
                product = jnp.dot(
                    table,
                    gathered[step, index, :, mode].reshape(width, lanes),
                    preferred_element_type=jnp.float32,
                )
                at = slice(mode * lanes, (mode + 1) * lanes)
                leaving[step, index, :, at] = product[:half].astype(jnp.bfloat16)
                kept[step, index, :, at] = product[half:]
            for side in range(pieces):
                middle_copy(step, index, other, side).start()

    def rotate_step(step):
        for side in range(pieces):
            for index, gather, other in sets:
                middle_copy(step, index, other, side).wait_recv()
                apart = (me // gather + side) % 2
                for core in (1, 0):
                    start = pl.multiple_of((2 * side + (me + core) % 2) * tile, tile)
                    rows = pl.ds(start, tile)
                    owner = apart * gather + core
                    real_in = []
                    imag_in = []
                    for k in range(modes):
                        at = slice(k * lanes, (k + 1) * lanes)
                        total = kept[step, index, rows, at] + arriving[
                            step, index, rows, at
                        ].astype(jnp.float32)
                        real_in.append(total[:q_local])
                        imag_in.append(total[q_local:])
                    for mode in range(modes):
                        real_out = jnp.zeros((q_local, lanes), jnp.float32)
                        imag_out = jnp.zeros((q_local, lanes), jnp.float32)
                        for k in range(modes):
                            vec_real = vectors[owner, (k * modes + mode) * parts]
                            vec_imag = vectors[owner, (k * modes + mode) * parts + 1]
                            real_out += real_in[k] * vec_real - imag_in[k] * vec_imag
                            imag_out += real_in[k] * vec_imag + imag_in[k] * vec_real
                        turned[turned_at(step, index, side, core), mode] = jnp.concatenate(
                            [real_out, imag_out], axis=0
                        ).astype(jnp.bfloat16)
                    send_last(step, index, gather, side, core)

    gather_step(steps[0])
    eigvec_all().wait_recv()
    for turn in range(len(near)):
        flat = all_eigvec[turn]
        for entry in range(entries):
            vectors[turn, entry] = jnp.broadcast_to(flat[:, entry : entry + 1], (q_local, lanes))
    send_first(steps[2])
    gather_step(steps[1])

    @pl.when(plane < planes - 1)
    def _():
        pl.semaphore_wait(above_sem, planes - 1 - plane)

    rotate_step(steps[0])
    send_first(steps[3])
    gather_step(steps[2])
    rotate_step(steps[1])
    gather_step(steps[3])
    rotate_step(steps[2])
    rotate_step(steps[3])

    lattice_all().wait_send()
    eigvec_all().wait_send()
    everything = gathered.at[:, :, pl.ds(0, (group - 1) * local_rp)]
    bundle(everything, first_send.at[0], first_recv.at[0, 0]).wait_send()
    bundle(leaving, middle_send.at[0], middle_recv.at[0, 0, 0]).wait_send()
    for index, gather, _ in sets:
        last_own(index, gather, me // gather % 2).wait()
    last_all().wait_recv()
    last_all().wait_send()


def spread_kernel(planes, held, out, rows_of, sems):
    _, modes, tile, lanes = held.shape
    blocks = held.shape[0] // planes
    q_local = tile // 2
    per_plane = modes * blocks * 2
    per_q = planes * per_plane

    def copies(source):
        return [
            pltpu.make_async_copy(
                rows_of.at[pl.ds(q * per_q + source * per_plane, per_plane)],
                out.at[pl.ds(q * per_q + source * per_plane, per_plane)],
                sems.at[source, q],
            )
            for q in range(q_local)
        ]

    for source in range(planes):
        for mode in range(modes):
            for block in range(blocks):
                values = held[source * blocks + block, mode].astype(jnp.float32)
                row = source * per_plane + (mode * blocks + block) * 2
                rows_of[pl.ds(row, q_local, stride=per_q), :] = values[:q_local]
                rows_of[pl.ds(row + 1, q_local, stride=per_q), :] = values[q_local:]
        for copy in copies(source):
            copy.start()
    for source in range(planes):
        for copy in copies(source):
            copy.wait()


def in_hbm(value):
    return pltpu.with_memory_space_constraint(value, pltpu.HBM)


def exchanged(coupling, rp_coords, degeneracy, qpoints, eigvec):
    n = lax.axis_size("rp")
    planes = lax.axis_size("re")
    local_rp, local_re, parts, modes, pairs = coupling.shape
    q_local = eigvec.shape[0]
    lanes = pairs // planes // n
    group = n // 2
    tile = parts * q_local
    half = group * tile
    width = group * local_rp * parts
    entries = parts * modes * modes
    near = 6
    gathered = pl.pallas_call(
        functools.partial(rotation_kernel, n, planes),
        out_shape=jax.ShapeDtypeStruct((planes * n, modes, tile, lanes), jnp.bfloat16),
        in_specs=[
            pl.BlockSpec(memory_space=pltpu.HBM),
            pl.BlockSpec(memory_space=pltpu.HBM),
            pl.BlockSpec(memory_space=pltpu.HBM),
            pl.BlockSpec(memory_space=pltpu.HBM),
            pl.BlockSpec(memory_space=pltpu.HBM),
        ],
        out_specs=pl.BlockSpec(memory_space=pl.ANY),
        scratch_shapes=[
            pltpu.VMEM(qpoints.shape, jnp.int32),
            pltpu.VMEM((planes, 2, group * local_rp, modes, parts, lanes), jnp.bfloat16),
            pltpu.VMEM((local_rp, modes, parts, pairs // planes), jnp.bfloat16),
            pltpu.VMEM((2, group, rp_coords.shape[0] + 1, local_rp), jnp.int32),
            pltpu.VMEM((modes * modes, parts, q_local), jnp.float32),
            pltpu.VMEM((near, q_local, lanes), jnp.float32),
            pltpu.VMEM((2, 2 * half, width), jnp.float32),
            pltpu.VMEM((near, entries, q_local, lanes), jnp.float32),
            pltpu.VMEM((planes, 2, half, modes * lanes), jnp.float32),
            pltpu.VMEM((planes, 2, half, modes * lanes), jnp.bfloat16),
            pltpu.VMEM((planes, 2, half, modes * lanes), jnp.bfloat16),
            pltpu.VMEM((planes * n, modes, tile, lanes), jnp.bfloat16),
            pltpu.SemaphoreType.DMA((17,)),
            pltpu.SemaphoreType.DMA((2,)),
            pltpu.SemaphoreType.DMA((2,)),
            pltpu.SemaphoreType.DMA((1,)),
            pltpu.SemaphoreType.DMA((planes, 2)),
            pltpu.SemaphoreType.DMA((1,)),
            pltpu.SemaphoreType.DMA((planes, 2, 2)),
            pltpu.SemaphoreType.DMA((1,)),
            pltpu.SemaphoreType.DMA((1,)),
            pltpu.SemaphoreType.REGULAR,
        ],
        compiler_params=pltpu.CompilerParams(
            collective_id=0, has_side_effects=True, vmem_limit_bytes=24 * 2**20
        ),
    )(
        in_hbm(jnp.swapaxes(coupling[:, 0], 1, 2)),
        in_hbm(rp_coords),
        in_hbm(degeneracy[None, :]),
        in_hbm(jnp.transpose(eigvec, (2, 3, 1, 0)).reshape(modes * modes, parts, q_local)),
        in_hbm(qpoints),
    )
    rows = q_local * planes * modes * n * parts
    spread = pl.pallas_call(
        functools.partial(spread_kernel, planes),
        out_shape=jax.ShapeDtypeStruct((rows, lanes), jnp.float32),
        in_specs=[pl.BlockSpec(memory_space=pltpu.VMEM)],
        out_specs=pl.BlockSpec(memory_space=pl.ANY),
        scratch_shapes=[
            pltpu.VMEM((rows, lanes), jnp.float32),
            pltpu.SemaphoreType.DMA((planes, q_local)),
        ],
        compiler_params=pltpu.CompilerParams(vmem_limit_bytes=24 * 2**20),
    )(gathered)
    spread = spread.reshape(q_local, planes, modes, n, parts, lanes)
    spread = jnp.transpose(spread, (0, 1, 4, 2, 3, 5))
    return spread.reshape(q_local, planes, parts, modes, n * lanes)


def fits(n, planes, coupling, eigvec):
    local_rp, local_re, parts, modes, pairs = coupling.shape
    return (
        local_re == 1
        and n == 8
        and planes == 4
        and local_rp * n == 128
        and parts * modes * modes <= 128
        and pairs // planes // n == 128
        and eigvec.shape[0] == 8
        and modes <= 8
    )


def either(coupling, rp_coords, degeneracy, qpoints, eigvec):
    if fits(lax.axis_size("rp"), lax.axis_size("re"), coupling, eigvec):
        return exchanged(coupling, rp_coords, degeneracy, qpoints, eigvec)
    return per_device(coupling, rp_coords, degeneracy, qpoints, eigvec)


def solution(mesh):
    return jax.shard_map(
        either,
        mesh=mesh,
        in_specs=(
            P("rp", "re", None, None, None),
            P(None, "rp"),
            P("rp"),
            P(),
            P("rp", None, None, None),
        ),
        out_specs=P("rp", None, None, None, "re"),
        check_vma=False,
    )
```

```python
import functools
import math

import jax
import jax.numpy as jnp
from jax import lax
from jax.experimental import pallas as pl
from jax.experimental.pallas import tpu as pltpu
from jax.sharding import PartitionSpec as P

QGRID = 16
MESH = pl.DeviceIdType.MESH


def phases(points, coords, degeneracy):
    turns = jnp.mod(points[0][:, None] * coords[0][None, :], QGRID)
    turns = turns + jnp.mod(points[1][:, None] * coords[1][None, :], QGRID)
    turns = turns + jnp.mod(points[2][:, None] * coords[2][None, :], QGRID)
    turns = jnp.mod(turns, QGRID)
    angles = turns.astype(jnp.float32) * (2.0 * math.pi / QGRID)
    weights = 1.0 / degeneracy.astype(jnp.float32)
    table = jnp.concatenate(
        [jnp.cos(angles) * weights[None, :], jnp.sin(angles) * weights[None, :]], axis=0
    )
    return table.astype(jnp.bfloat16)


def combine(table, coupling):
    point_count = table.shape[0] // 2
    product = jnp.dot(
        table, coupling.reshape(coupling.shape[0], -1), preferred_element_type=jnp.float32
    )
    product = product.reshape((2, point_count) + coupling.shape[1:])
    real_part = product[0, :, :, 0] - product[1, :, :, 1]
    imag_part = product[0, :, :, 1] + product[1, :, :, 0]
    return jnp.stack([real_part, imag_part], axis=2)


def mode_mix(values, matrix):
    return jnp.einsum("qrkp,qkn->qrnp", values, matrix, precision=lax.Precision.HIGHEST)


def rotate(summed, eigvec):
    real_in = summed[:, :, 0]
    imag_in = summed[:, :, 1]
    vec_real = eigvec[:, 0]
    vec_imag = eigvec[:, 1]
    real_out = mode_mix(real_in, vec_real) - mode_mix(imag_in, vec_imag)
    imag_out = mode_mix(real_in, vec_imag) + mode_mix(imag_in, vec_real)
    return jnp.stack([real_out, imag_out], axis=2)


def to_owners(all_points):
    return lax.all_to_all(all_points, "rp", split_axis=0, concat_axis=3, tiled=True)


def per_device(coupling, rp_coords, degeneracy, qpoints, eigvec):
    stacked = jnp.concatenate([rp_coords, degeneracy[None, :]], axis=0)
    lattice = lax.all_gather(stacked, "rp", axis=1, tiled=True)
    table = phases(qpoints, lattice[:3], lattice[3])
    rp_count = lax.axis_size("rp")
    re_count = lax.axis_size("re")
    local_rp, local_re, parts, mode_count, pair_count = coupling.shape
    q_local = eigvec.shape[0]
    pair_share = pair_count // re_count
    block_cols = mode_count * pair_share
    inner = block_cols // rp_count
    reordered = coupling.reshape(local_rp, local_re, parts, mode_count, re_count, pair_share)
    reordered = jnp.swapaxes(reordered, 3, 4)
    reordered = reordered.reshape(local_rp, local_re, parts, re_count, rp_count, inner)
    reordered = jnp.swapaxes(reordered, 3, 4)
    reordered = reordered.reshape(local_rp, local_re, parts, rp_count * re_count * inner)
    moved = lax.all_to_all(
        lax.all_to_all(reordered, "rp", split_axis=3, concat_axis=0, tiled=True),
        "re",
        split_axis=3,
        concat_axis=1,
        tiled=True,
    )
    all_points = combine(table, moved)
    summed = to_owners(all_points)
    summed = summed.reshape(q_local, summed.shape[1], parts, mode_count, pair_share)
    return rotate(summed, eigvec)


def column_of(angle):
    return [math.cos(2.0 * math.pi * (step - angle) / QGRID) for step in range(QGRID)]


def pick(turns, values):
    picked = jnp.full(turns.shape, values[0], jnp.float32)
    for step in range(1, QGRID):
        picked = jnp.where(turns == step, jnp.float32(values[step]), picked)
    return picked


def flip(index, bits):
    for bit in (1, 2, 4):
        if bits & bit:
            index = index + bit - 2 * bit * (index // bit % 2)
    return index


def place(index, gather):
    return 2 * (index // gather % 2) + index % 2


ORDER = ((2, 3, 1, 0), (3, 2, 0, 1), (0, 1, 3, 2), (0, 1, 2, 3))


def aim(plane, turn):
    target = ORDER[0][turn]
    for level in range(1, len(ORDER)):
        target = jnp.where(plane == level, ORDER[level][turn], target)
    return target


def rotation_kernel(
    n,
    planes,
    coupling,
    coords,
    degeneracy,
    eigvec,
    points_in,
    out,
    points,
    gathered,
    early,
    all_lattice,
    own_eigvec,
    all_eigvec,
    table_rows,
    vectors,
    kept,
    leaving,
    arriving,
    turned,
    own_sem,
    small_send,
    small_recv,
    first_send,
    first_recv,
    middle_send,
    middle_recv,
    last_send,
    last_recv,
    above_sem,
):
    me = lax.axis_index("rp")
    plane = lax.axis_index("re")
    local_rp, modes, parts, pairs = coupling.shape
    share = pairs // planes
    lanes = gathered.shape[-1]
    q_local = eigvec.shape[-1]
    group = 4
    tile = parts * q_local
    half = group * tile
    pieces = 4
    width = group * local_rp * parts
    steps = tuple(range(planes))
    aims = [aim(plane, turn) for turn in steps]
    sets = ((0, 4, 2), (1, 2, 4))
    near = (0, 1, 2, 3, 4, 5)

    barrier = pltpu.get_barrier_semaphore()

    def greet(semaphore, bits, level):
        pl.semaphore_signal(
            semaphore,
            inc=1,
            device_id={"rp": flip(me, bits), "re": level},
            device_id_type=MESH,
        )

    def local(source, target, index):
        return pltpu.make_async_copy(source, target, own_sem.at[index])

    def remote(source, target, send, recv, bits, step=0):
        return pltpu.make_async_remote_copy(
            src_ref=source,
            dst_ref=target,
            send_sem=send,
            recv_sem=recv,
            device_id={"rp": flip(me, bits), "re": flip(plane, step)},
            device_id_type=MESH,
        )

    def members(gather):
        return (gather + 1, gather, 1)

    def lattice_copies():
        return [
            remote(
                all_lattice.at[index, place(me, gather)],
                all_lattice.at[index, place(me, gather)],
                small_send.at[0],
                small_recv.at[0],
                bits,
            )
            for index, gather, _ in sets
            for turn, bits in enumerate(members(gather))
        ]

    def eigvec_copies():
        return [
            remote(
                all_eigvec.at[0],
                all_eigvec.at[turn],
                small_send.at[1],
                small_recv.at[1],
                bits,
            )
            for turn, bits in enumerate(near)
            if bits
        ]

    def bundle(held, send, recv):
        return remote(held, held, send, recv, 1)

    def lattice_all():
        held = all_lattice.at[:, pl.ds(0, group - 1)]
        return bundle(held, small_send.at[0], small_recv.at[0])

    def eigvec_all():
        return bundle(all_eigvec.at[pl.ds(1, len(near) - 1)], small_send.at[1], small_recv.at[1])

    def first_all(step, index):
        held = gathered.at[step, index, pl.ds(0, (group - 1) * local_rp)]
        return bundle(held, first_send.at[0], first_recv.at[step, index])

    def lattice_own():
        copies = []
        for index, gather, _ in sets:
            held = all_lattice.at[index, place(me, gather)]
            copies.append(local(coords, held.at[pl.ds(0, 3)], 2 * index))
            copies.append(local(degeneracy, held.at[pl.ds(3, 1)], 2 * index + 1))
        return copies

    def early_own():
        start = pl.multiple_of(aims[0] * share, share)
        return local(coupling.at[:, :, :, pl.ds(start, share)], early, 16)

    eigvec_own = local(eigvec, own_eigvec, 4)
    points_own = local(points_in, points, 15)

    def piece(step, index, owner, gather):
        block = index * group + place(owner, gather)
        if step == steps[0]:
            return early.at[:, :, :, pl.ds(pl.multiple_of(block * lanes, lanes), lanes)]
        block = aims[step] * 2 * group + block
        return coupling.at[:, :, :, pl.ds(pl.multiple_of(block * lanes, lanes), lanes)]

    def landing(step, index, gather):
        return gathered.at[step, index, pl.ds(place(me, gather) * local_rp, local_rp)]

    def first_copy(step, index, gather, bits):
        return remote(
            piece(step, index, flip(me, bits), gather),
            landing(step, index, gather),
            first_send.at[0],
            first_recv.at[step, index],
            bits,
        )

    def first_own(step, index, gather):
        return local(
            piece(step, index, me, gather),
            landing(step, index, gather),
            5 + 2 * step + index,
        )

    def send_first(step, turns=(0, 1, 2)):
        for turn in turns:
            for index, gather, _ in sets:
                first_copy(step, index, gather, members(gather)[turn]).start()
        if 2 in turns:
            for index, gather, _ in sets:
                first_own(step, index, gather).start()

    def middle_copy(step, index, other, side):
        rows = pl.ds(side * (half // pieces), half // pieces)
        return remote(
            leaving.at[step, index, rows],
            arriving.at[step, index, rows],
            middle_send.at[0],
            middle_recv.at[step, index, side],
            other,
        )

    def final_block(index, origin, gather):
        return index * group + place(origin, gather)

    def turned_at(step, index, side, core):
        return ((step * 2 + index) * 2 + side) * 2 + core

    def last_copy(step, index, gather, side, core):
        source = turned.at[turned_at(step, index, side, core)]
        target = out.at[plane * n + final_block(index, me, gather)]
        owner = me + core - me % 2 + gather * (side - me // gather % 2)
        return pltpu.make_async_remote_copy(
            src_ref=source,
            dst_ref=target,
            send_sem=last_send.at[0],
            recv_sem=last_recv.at[0],
            device_id={"rp": owner, "re": aims[step]},
            device_id_type=MESH,
        )

    def last_all():
        count = n * planes - len(sets)
        return pltpu.make_async_remote_copy(
            src_ref=turned.at[pl.ds(0, count)],
            dst_ref=out.at[pl.ds(0, count)],
            send_sem=last_send.at[0],
            recv_sem=last_recv.at[0],
            device_id={"rp": flip(me, 1)},
            device_id_type=MESH,
        )

    def last_own(index, gather, side):
        return local(
            turned.at[turned_at(planes - 1, index, side, me % 2)],
            out.at[plane * n + final_block(index, me, gather)],
            13 + index,
        )

    def send_last(step, index, gather, side, core):
        if step < planes - 1:
            last_copy(step, index, gather, side, core).start()
            return
        same = jnp.logical_and(me // gather % 2 == side, me % 2 == core)

        @pl.when(same)
        def _():
            last_own(index, gather, side).start()

        @pl.when(jnp.logical_not(same))
        def _():
            last_copy(step, index, gather, side, core).start()

    early_own().start()
    for copy in lattice_own():
        copy.start()
    points_own.start()
    eigvec_own.start()
    for bits in near[1:]:
        greet(barrier, bits, plane)
    for ahead in range(1, planes):

        @pl.when(plane + ahead < planes)
        def _():
            for bits in near:
                greet(barrier, bits, plane + ahead)

    for copy in lattice_own():
        copy.wait()
    early_own().wait()
    pl.semaphore_wait(barrier, len(near) - 1 + len(near) * plane)
    for copy in lattice_copies():
        copy.start()
    send_first(steps[0])
    for behind in range(1, planes):

        @pl.when(plane >= behind)
        def _():
            greet(above_sem, 0, plane - behind)
    eigvec_own.wait()
    entries = modes * modes * parts
    all_eigvec[0, :, :entries] = own_eigvec[...].reshape(entries, q_local).T
    for copy in eigvec_copies():
        copy.start()
    send_first(steps[1])

    points_own.wait()
    lattice_all().wait_recv()

    columns = lax.broadcasted_iota(jnp.int32, (group * local_rp, width), 1)
    repeat = columns // parts == lax.broadcasted_iota(jnp.int32, (group * local_rp, width), 0)
    repeat = repeat.astype(jnp.bfloat16)

    def twice(index):
        row = jnp.concatenate([all_lattice[index, slot] for slot in range(group)], axis=1)
        row = row.astype(jnp.float32).astype(jnp.bfloat16)
        return jnp.dot(row, repeat, preferred_element_type=jnp.float32)

    q_count = n * q_local
    real_part = lax.broadcasted_iota(jnp.int32, (q_count, width), 1) % parts == 0
    tables = []
    for index, gather, other in sets:
        lattice = twice(index)
        turns = lax.dot_general(
            points[...].astype(jnp.float32).astype(jnp.bfloat16),
            lattice[:3].astype(jnp.bfloat16),
            (((0,), (0,)), ((), ())),
            preferred_element_type=jnp.float32,
        )
        turns = turns.astype(jnp.int32) & (QGRID - 1)
        weights = 1.0 / lattice[3:]
        cos = pick(turns, column_of(0.0)) * weights
        sin = pick(turns, column_of(QGRID / 4)) * weights
        to_real = jnp.where(real_part, cos, -sin)
        to_imag = jnp.where(real_part, sin, cos)
        mine = me // other % 2
        for owner in range(n):
            across = owner // other % 2
            apart = across + mine - 2 * across * mine
            row = pl.multiple_of((1 - apart) * half + place(owner, gather) * tile, tile)
            rows = slice(owner * q_local, (owner + 1) * q_local)
            table_rows[index, pl.ds(row, q_local), :] = to_real[rows]
            table_rows[index, pl.ds(row + q_local, q_local), :] = to_imag[rows]

    def gather_step(step):
        for index, gather, other in sets:
            first_own(step, index, gather).wait()
            first_all(step, index).wait_recv()
            table = table_rows[index].astype(jnp.bfloat16)
            for mode in range(modes):
                product = jnp.dot(
                    table,
                    gathered[step, index, :, mode].reshape(width, lanes),
                    preferred_element_type=jnp.float32,
                )
                at = slice(mode * lanes, (mode + 1) * lanes)
                leaving[step, index, :, at] = product[:half].astype(jnp.bfloat16)
                kept[step, index, :, at] = product[half:]
            for side in range(pieces):
                middle_copy(step, index, other, side).start()

    def rotate_step(step):
        for piece_at in range(pieces):
            for index, gather, other in sets:
                side = piece_at // 2
                middle_copy(step, index, other, piece_at).wait_recv()
                apart = (me // gather + side) % 2
                for core in (0,):
                    start = pl.multiple_of(piece_at * tile, tile)
                    rows = pl.ds(start, tile)
                    owner = apart * gather + (me + piece_at) % 2
                    real_in = []
                    imag_in = []
                    for k in range(modes):
                        at = slice(k * lanes, (k + 1) * lanes)
                        total = kept[step, index, rows, at] + arriving[
                            step, index, rows, at
                        ].astype(jnp.float32)
                        real_in.append(total[:q_local])
                        imag_in.append(total[q_local:])
                    for mode in range(modes):
                        real_out = jnp.zeros((q_local, lanes), jnp.float32)
                        imag_out = jnp.zeros((q_local, lanes), jnp.float32)
                        for k in range(modes):
                            vec_real = vectors[owner, (k * modes + mode) * parts]
                            vec_imag = vectors[owner, (k * modes + mode) * parts + 1]
                            real_out += real_in[k] * vec_real - imag_in[k] * vec_imag
                            imag_out += real_in[k] * vec_imag + imag_in[k] * vec_real
                        turned[turned_at(step, index, side, piece_at % 2), mode] = jnp.concatenate(
                            [real_out, imag_out], axis=0
                        ).astype(jnp.bfloat16)
                    send_last(step, index, gather, side, piece_at % 2)

    gather_step(steps[0])
    eigvec_all().wait_recv()
    for turn in range(len(near)):
        flat = all_eigvec[turn]
        for entry in range(entries):
            vectors[turn, entry] = jnp.broadcast_to(flat[:, entry : entry + 1], (q_local, lanes))
    send_first(steps[2])
    gather_step(steps[1])

    @pl.when(plane < planes - 1)
    def _():
        pl.semaphore_wait(above_sem, planes - 1 - plane)

    rotate_step(steps[0])
    send_first(steps[3])
    gather_step(steps[2])
    rotate_step(steps[1])
    gather_step(steps[3])
    rotate_step(steps[2])
    rotate_step(steps[3])

    lattice_all().wait_send()
    eigvec_all().wait_send()
    everything = gathered.at[:, :, pl.ds(0, (group - 1) * local_rp)]
    bundle(everything, first_send.at[0], first_recv.at[0, 0]).wait_send()
    bundle(leaving, middle_send.at[0], middle_recv.at[0, 0, 0]).wait_send()
    for index, gather, _ in sets:
        last_own(index, gather, me // gather % 2).wait()
    last_all().wait_recv()
    last_all().wait_send()


def spread_kernel(planes, held, out, rows_of, sems):
    _, modes, tile, lanes = held.shape
    blocks = held.shape[0] // planes
    q_local = tile // 2
    per_plane = modes * blocks * 2
    per_q = rows_of.shape[0] // q_local
    by_q = rows_of.reshape(q_local, per_q, lanes)

    def spread(source):
        rows = pl.ds(source * per_plane, per_plane)
        return pltpu.make_async_copy(by_q.at[:, rows], out.at[:, rows], sems.at[source])

    for source in range(planes):
        for mode in range(modes):
            for block in range(blocks):
                values = held[source * blocks + block, mode].astype(jnp.float32)
                row = source * per_plane + (mode * blocks + block) * 2
                rows_of[pl.ds(row, q_local, stride=per_q), :] = values[:q_local]
                rows_of[pl.ds(row + 1, q_local, stride=per_q), :] = values[q_local:]
        spread(source).start()
    for source in range(planes):
        spread(source).wait()


def in_hbm(value):
    return pltpu.with_memory_space_constraint(value, pltpu.HBM)


def exchanged(coupling, rp_coords, degeneracy, qpoints, eigvec):
    n = lax.axis_size("rp")
    planes = lax.axis_size("re")
    local_rp, local_re, parts, modes, pairs = coupling.shape
    q_local = eigvec.shape[0]
    lanes = pairs // planes // n
    group = n // 2
    tile = parts * q_local
    half = group * tile
    width = group * local_rp * parts
    entries = parts * modes * modes
    near = 6
    gathered = pl.pallas_call(
        functools.partial(rotation_kernel, n, planes),
        out_shape=jax.ShapeDtypeStruct((planes * n, modes, tile, lanes), jnp.bfloat16),
        in_specs=[
            pl.BlockSpec(memory_space=pltpu.HBM),
            pl.BlockSpec(memory_space=pltpu.HBM),
            pl.BlockSpec(memory_space=pltpu.HBM),
            pl.BlockSpec(memory_space=pltpu.HBM),
            pl.BlockSpec(memory_space=pltpu.HBM),
        ],
        out_specs=pl.BlockSpec(memory_space=pl.ANY),
        scratch_shapes=[
            pltpu.VMEM(qpoints.shape, jnp.int32),
            pltpu.VMEM((planes, 2, group * local_rp, modes, parts, lanes), jnp.bfloat16),
            pltpu.VMEM((local_rp, modes, parts, pairs // planes), jnp.bfloat16),
            pltpu.VMEM((2, group, rp_coords.shape[0] + 1, local_rp), jnp.int32),
            pltpu.VMEM((modes * modes, parts, q_local), jnp.float32),
            pltpu.VMEM((near, q_local, lanes), jnp.float32),
            pltpu.VMEM((2, 2 * half, width), jnp.float32),
            pltpu.VMEM((near, entries, q_local, lanes), jnp.float32),
            pltpu.VMEM((planes, 2, half, modes * lanes), jnp.float32),
            pltpu.VMEM((planes, 2, half, modes * lanes), jnp.bfloat16),
            pltpu.VMEM((planes, 2, half, modes * lanes), jnp.bfloat16),
            pltpu.VMEM((planes * n, modes, tile, lanes), jnp.bfloat16),
            pltpu.SemaphoreType.DMA((17,)),
            pltpu.SemaphoreType.DMA((2,)),
            pltpu.SemaphoreType.DMA((2,)),
            pltpu.SemaphoreType.DMA((1,)),
            pltpu.SemaphoreType.DMA((planes, 2)),
            pltpu.SemaphoreType.DMA((1,)),
            pltpu.SemaphoreType.DMA((planes, 2, 4)),
            pltpu.SemaphoreType.DMA((1,)),
            pltpu.SemaphoreType.DMA((1,)),
            pltpu.SemaphoreType.REGULAR,
        ],
        compiler_params=pltpu.CompilerParams(
            collective_id=0, has_side_effects=True, vmem_limit_bytes=24 * 2**20
        ),
    )(
        in_hbm(jnp.swapaxes(coupling[:, 0], 1, 2)),
        in_hbm(rp_coords),
        in_hbm(degeneracy[None, :]),
        in_hbm(jnp.transpose(eigvec, (2, 3, 1, 0)).reshape(modes * modes, parts, q_local)),
        in_hbm(qpoints),
    )
    rows = planes * modes * n * parts
    spread = pl.pallas_call(
        functools.partial(spread_kernel, planes),
        out_shape=jax.ShapeDtypeStruct((q_local, rows, lanes), jnp.float32),
        in_specs=[pl.BlockSpec(memory_space=pltpu.VMEM)],
        out_specs=pl.BlockSpec(memory_space=pl.ANY),
        scratch_shapes=[
            pltpu.VMEM((q_local * (rows + 8), lanes), jnp.float32),
            pltpu.SemaphoreType.DMA((planes,)),
        ],
        compiler_params=pltpu.CompilerParams(vmem_limit_bytes=24 * 2**20),
    )(gathered)
    spread = spread.reshape(q_local, planes, modes, n, parts, lanes)
    spread = jnp.transpose(spread, (0, 1, 4, 2, 3, 5))
    return spread.reshape(q_local, planes, parts, modes, n * lanes)


def fits(n, planes, coupling, eigvec):
    local_rp, local_re, parts, modes, pairs = coupling.shape
    return (
        local_re == 1
        and n == 8
        and planes == 4
        and local_rp * n == 128
        and parts * modes * modes <= 128
        and pairs // planes // n == 128
        and eigvec.shape[0] == 8
        and modes <= 8
    )


def either(coupling, rp_coords, degeneracy, qpoints, eigvec):
    if fits(lax.axis_size("rp"), lax.axis_size("re"), coupling, eigvec):
        return exchanged(coupling, rp_coords, degeneracy, qpoints, eigvec)
    return per_device(coupling, rp_coords, degeneracy, qpoints, eigvec)


def solution(mesh):
    return jax.shard_map(
        either,
        mesh=mesh,
        in_specs=(
            P("rp", "re", None, None, None),
            P(None, "rp"),
            P("rp"),
            P(),
            P("rp", None, None, None),
        ),
        out_specs=P("rp", None, None, None, "re"),
        check_vma=False,
    )
```

```python
import functools
import math

import jax
import jax.numpy as jnp
from jax import lax
from jax.experimental import pallas as pl
from jax.experimental.pallas import tpu as pltpu
from jax.sharding import PartitionSpec as P

QGRID = 16
MESH = pl.DeviceIdType.MESH


def phases(points, coords, degeneracy):
    turns = jnp.mod(points[0][:, None] * coords[0][None, :], QGRID)
    turns = turns + jnp.mod(points[1][:, None] * coords[1][None, :], QGRID)
    turns = turns + jnp.mod(points[2][:, None] * coords[2][None, :], QGRID)
    turns = jnp.mod(turns, QGRID)
    angles = turns.astype(jnp.float32) * (2.0 * math.pi / QGRID)
    weights = 1.0 / degeneracy.astype(jnp.float32)
    table = jnp.concatenate(
        [jnp.cos(angles) * weights[None, :], jnp.sin(angles) * weights[None, :]], axis=0
    )
    return table.astype(jnp.bfloat16)


def combine(table, coupling):
    point_count = table.shape[0] // 2
    product = jnp.dot(
        table, coupling.reshape(coupling.shape[0], -1), preferred_element_type=jnp.float32
    )
    product = product.reshape((2, point_count) + coupling.shape[1:])
    real_part = product[0, :, :, 0] - product[1, :, :, 1]
    imag_part = product[0, :, :, 1] + product[1, :, :, 0]
    return jnp.stack([real_part, imag_part], axis=2)


def mode_mix(values, matrix):
    return jnp.einsum("qrkp,qkn->qrnp", values, matrix, precision=lax.Precision.HIGHEST)


def rotate(summed, eigvec):
    real_in = summed[:, :, 0]
    imag_in = summed[:, :, 1]
    vec_real = eigvec[:, 0]
    vec_imag = eigvec[:, 1]
    real_out = mode_mix(real_in, vec_real) - mode_mix(imag_in, vec_imag)
    imag_out = mode_mix(real_in, vec_imag) + mode_mix(imag_in, vec_real)
    return jnp.stack([real_out, imag_out], axis=2)


def to_owners(all_points):
    return lax.all_to_all(all_points, "rp", split_axis=0, concat_axis=3, tiled=True)


def per_device(coupling, rp_coords, degeneracy, qpoints, eigvec):
    stacked = jnp.concatenate([rp_coords, degeneracy[None, :]], axis=0)
    lattice = lax.all_gather(stacked, "rp", axis=1, tiled=True)
    table = phases(qpoints, lattice[:3], lattice[3])
    rp_count = lax.axis_size("rp")
    re_count = lax.axis_size("re")
    local_rp, local_re, parts, mode_count, pair_count = coupling.shape
    q_local = eigvec.shape[0]
    pair_share = pair_count // re_count
    block_cols = mode_count * pair_share
    inner = block_cols // rp_count
    reordered = coupling.reshape(local_rp, local_re, parts, mode_count, re_count, pair_share)
    reordered = jnp.swapaxes(reordered, 3, 4)
    reordered = reordered.reshape(local_rp, local_re, parts, re_count, rp_count, inner)
    reordered = jnp.swapaxes(reordered, 3, 4)
    reordered = reordered.reshape(local_rp, local_re, parts, rp_count * re_count * inner)
    moved = lax.all_to_all(
        lax.all_to_all(reordered, "rp", split_axis=3, concat_axis=0, tiled=True),
        "re",
        split_axis=3,
        concat_axis=1,
        tiled=True,
    )
    all_points = combine(table, moved)
    summed = to_owners(all_points)
    summed = summed.reshape(q_local, summed.shape[1], parts, mode_count, pair_share)
    return rotate(summed, eigvec)


def column_of(angle):
    return [math.cos(2.0 * math.pi * (step - angle) / QGRID) for step in range(QGRID)]


def pick(turns, values):
    picked = jnp.full(turns.shape, values[0], jnp.float32)
    for step in range(1, QGRID):
        picked = jnp.where(turns == step, jnp.float32(values[step]), picked)
    return picked


def flip(index, bits):
    for bit in (1, 2, 4):
        if bits & bit:
            index = index + bit - 2 * bit * (index // bit % 2)
    return index


def place(index, gather):
    return 2 * (index // gather % 2) + index % 2


ORDER = ((2, 3, 1, 0), (3, 2, 0, 1), (0, 1, 3, 2), (0, 1, 2, 3))


def aim(plane, turn):
    target = ORDER[0][turn]
    for level in range(1, len(ORDER)):
        target = jnp.where(plane == level, ORDER[level][turn], target)
    return target


def rotation_kernel(
    n,
    planes,
    coupling,
    coords,
    degeneracy,
    eigvec,
    points_in,
    out,
    points,
    gathered,
    early,
    all_lattice,
    own_eigvec,
    all_eigvec,
    table_rows,
    vectors,
    kept,
    leaving,
    arriving,
    turned,
    own_sem,
    small_send,
    small_recv,
    first_send,
    first_recv,
    middle_send,
    middle_recv,
    last_send,
    last_recv,
    above_sem,
):
    me = lax.axis_index("rp")
    plane = lax.axis_index("re")
    local_rp, modes, parts, pairs = coupling.shape
    share = pairs // planes
    lanes = gathered.shape[-1]
    q_local = eigvec.shape[-1]
    group = 4
    tile = parts * q_local
    half = group * tile
    pieces = 4
    width = group * local_rp * parts
    steps = tuple(range(planes))
    aims = [aim(plane, turn) for turn in steps]
    sets = ((0, 4, 2), (1, 2, 4))
    near = (0, 1, 2, 3, 4, 5)

    barrier = pltpu.get_barrier_semaphore()

    def greet(semaphore, bits, level):
        pl.semaphore_signal(
            semaphore,
            inc=1,
            device_id={"rp": flip(me, bits), "re": level},
            device_id_type=MESH,
        )

    def local(source, target, index):
        return pltpu.make_async_copy(source, target, own_sem.at[index])

    def remote(source, target, send, recv, bits, step=0):
        return pltpu.make_async_remote_copy(
            src_ref=source,
            dst_ref=target,
            send_sem=send,
            recv_sem=recv,
            device_id={"rp": flip(me, bits), "re": flip(plane, step)},
            device_id_type=MESH,
        )

    def members(gather):
        return (gather + 1, gather, 1)

    def lattice_copies():
        return [
            remote(
                all_lattice.at[index, place(me, gather)],
                all_lattice.at[index, place(me, gather)],
                small_send.at[0],
                small_recv.at[0],
                bits,
            )
            for index, gather, _ in sets
            for turn, bits in enumerate(members(gather))
        ]

    def eigvec_copies():
        return [
            remote(
                all_eigvec.at[0],
                all_eigvec.at[turn],
                small_send.at[1],
                small_recv.at[1],
                bits,
            )
            for turn, bits in enumerate(near)
            if bits
        ]

    def bundle(held, send, recv):
        return remote(held, held, send, recv, 1)

    def lattice_all():
        held = all_lattice.at[:, pl.ds(0, group - 1)]
        return bundle(held, small_send.at[0], small_recv.at[0])

    def eigvec_all():
        return bundle(all_eigvec.at[pl.ds(1, len(near) - 1)], small_send.at[1], small_recv.at[1])

    def first_all(step, index):
        held = gathered.at[step, index, pl.ds(0, (group - 1) * local_rp)]
        return bundle(held, first_send.at[0], first_recv.at[step, index])

    def lattice_own():
        copies = []
        for index, gather, _ in sets:
            held = all_lattice.at[index, place(me, gather)]
            copies.append(local(coords, held.at[pl.ds(0, 3)], 2 * index))
            copies.append(local(degeneracy, held.at[pl.ds(3, 1)], 2 * index + 1))
        return copies

    def early_own():
        start = pl.multiple_of(aims[0] * share, share)
        return local(coupling.at[:, :, :, pl.ds(start, share)], early, 16)

    eigvec_own = local(eigvec, own_eigvec, 4)
    points_own = local(points_in, points, 15)

    def piece(step, index, owner, gather):
        block = index * group + place(owner, gather)
        if step == steps[0]:
            return early.at[:, :, :, pl.ds(pl.multiple_of(block * lanes, lanes), lanes)]
        block = aims[step] * 2 * group + block
        return coupling.at[:, :, :, pl.ds(pl.multiple_of(block * lanes, lanes), lanes)]

    def landing(step, index, gather):
        return gathered.at[step, index, pl.ds(place(me, gather) * local_rp, local_rp)]

    def first_copy(step, index, gather, bits):
        return remote(
            piece(step, index, flip(me, bits), gather),
            landing(step, index, gather),
            first_send.at[0],
            first_recv.at[step, index],
            bits,
        )

    def first_own(step, index, gather):
        return local(
            piece(step, index, me, gather),
            landing(step, index, gather),
            5 + 2 * step + index,
        )

    def send_first(step, turns=(0, 1, 2)):
        for turn in turns:
            for index, gather, _ in sets:
                first_copy(step, index, gather, members(gather)[turn]).start()
        if 2 in turns:
            for index, gather, _ in sets:
                first_own(step, index, gather).start()

    def middle_copy(step, index, other, side):
        rows = pl.ds(side * (half // pieces), half // pieces)
        return remote(
            leaving.at[step, index, rows],
            arriving.at[step, index, rows],
            middle_send.at[0],
            middle_recv.at[step, index, side],
            other,
        )

    def final_block(index, origin, gather):
        return index * group + place(origin, gather)

    def turned_at(step, index, side, core):
        return ((step * 2 + index) * 2 + side) * 2 + core

    def last_copy(step, index, gather, side, core):
        source = turned.at[turned_at(step, index, side, core)]
        target = out.at[plane * n + final_block(index, me, gather)]
        owner = me + core - me % 2 + gather * (side - me // gather % 2)
        return pltpu.make_async_remote_copy(
            src_ref=source,
            dst_ref=target,
            send_sem=last_send.at[0],
            recv_sem=last_recv.at[0],
            device_id={"rp": owner, "re": aims[step]},
            device_id_type=MESH,
        )

    def last_all():
        count = n * planes - len(sets)
        return pltpu.make_async_remote_copy(
            src_ref=turned.at[pl.ds(0, count)],
            dst_ref=out.at[pl.ds(0, count)],
            send_sem=last_send.at[0],
            recv_sem=last_recv.at[0],
            device_id={"rp": flip(me, 1)},
            device_id_type=MESH,
        )

    def last_own(index, gather, side):
        return local(
            turned.at[turned_at(planes - 1, index, side, me % 2)],
            out.at[plane * n + final_block(index, me, gather)],
            13 + index,
        )

    def send_last(step, index, gather, side, core):
        if step < planes - 1:
            last_copy(step, index, gather, side, core).start()
            return
        same = jnp.logical_and(me // gather % 2 == side, me % 2 == core)

        @pl.when(same)
        def _():
            last_own(index, gather, side).start()

        @pl.when(jnp.logical_not(same))
        def _():
            last_copy(step, index, gather, side, core).start()

    for bits in near[1:]:
        greet(barrier, bits, plane)
    for ahead in range(1, planes):

        @pl.when(plane + ahead < planes)
        def _():
            for bits in near:
                greet(barrier, bits, plane + ahead)

    for copy in lattice_own():
        copy.start()
    early_own().start()
    points_own.start()
    eigvec_own.start()
    for copy in lattice_own():
        copy.wait()
    early_own().wait()
    pl.semaphore_wait(barrier, len(near) - 1 + len(near) * plane)
    for copy in lattice_copies():
        copy.start()
    send_first(steps[0])
    eigvec_own.wait()
    entries = modes * modes * parts
    all_eigvec[0, :, :entries] = own_eigvec[...].reshape(entries, q_local).T
    for copy in eigvec_copies():
        copy.start()
    send_first(steps[1])
    for behind in range(1, planes):

        @pl.when(plane >= behind)
        def _():
            greet(above_sem, 0, plane - behind)

    points_own.wait()
    lattice_all().wait_recv()

    columns = lax.broadcasted_iota(jnp.int32, (group * local_rp, width), 1)
    repeat = columns // parts == lax.broadcasted_iota(jnp.int32, (group * local_rp, width), 0)
    repeat = repeat.astype(jnp.bfloat16)

    def twice(index):
        row = jnp.concatenate([all_lattice[index, slot] for slot in range(group)], axis=1)
        row = row.astype(jnp.float32).astype(jnp.bfloat16)
        return jnp.dot(row, repeat, preferred_element_type=jnp.float32)

    q_count = n * q_local
    real_part = lax.broadcasted_iota(jnp.int32, (q_count, width), 1) % parts == 0
    tables = []
    for index, gather, other in sets:
        lattice = twice(index)
        turns = lax.dot_general(
            points[...].astype(jnp.float32).astype(jnp.bfloat16),
            lattice[:3].astype(jnp.bfloat16),
            (((0,), (0,)), ((), ())),
            preferred_element_type=jnp.float32,
        )
        turns = turns.astype(jnp.int32) & (QGRID - 1)
        weights = 1.0 / lattice[3:]
        cos = pick(turns, column_of(0.0)) * weights
        sin = pick(turns, column_of(QGRID / 4)) * weights
        to_real = jnp.where(real_part, cos, -sin)
        to_imag = jnp.where(real_part, sin, cos)
        mine = me // other % 2
        for owner in range(n):
            across = owner // other % 2
            apart = across + mine - 2 * across * mine
            row = pl.multiple_of((1 - apart) * half + place(owner, gather) * tile, tile)
            rows = slice(owner * q_local, (owner + 1) * q_local)
            table_rows[index, pl.ds(row, q_local), :] = to_real[rows]
            table_rows[index, pl.ds(row + q_local, q_local), :] = to_imag[rows]

    def gather_step(step):
        for index, gather, other in sets:
            first_own(step, index, gather).wait()
            first_all(step, index).wait_recv()
            table = table_rows[index].astype(jnp.bfloat16)
            for mode in range(modes):
                product = jnp.dot(
                    table,
                    gathered[step, index, :, mode].reshape(width, lanes),
                    preferred_element_type=jnp.float32,
                )
                at = slice(mode * lanes, (mode + 1) * lanes)
                leaving[step, index, :, at] = product[:half].astype(jnp.bfloat16)
                kept[step, index, :, at] = product[half:]
            for side in range(pieces):
                middle_copy(step, index, other, side).start()

    def rotate_step(step):
        for piece_at in range(pieces):
            for index, gather, other in sets:
                side = piece_at // 2
                middle_copy(step, index, other, piece_at).wait_recv()
                apart = (me // gather + side) % 2
                for core in (0,):
                    start = pl.multiple_of(piece_at * tile, tile)
                    rows = pl.ds(start, tile)
                    owner = apart * gather + (me + piece_at) % 2
                    real_in = []
                    imag_in = []
                    for k in range(modes):
                        at = slice(k * lanes, (k + 1) * lanes)
                        total = kept[step, index, rows, at] + arriving[
                            step, index, rows, at
                        ].astype(jnp.float32)
                        real_in.append(total[:q_local])
                        imag_in.append(total[q_local:])
                    for mode in range(modes):
                        real_out = jnp.zeros((q_local, lanes), jnp.float32)
                        imag_out = jnp.zeros((q_local, lanes), jnp.float32)
                        for k in range(modes):
                            vec_real = vectors[owner, (k * modes + mode) * parts]
                            vec_imag = vectors[owner, (k * modes + mode) * parts + 1]
                            real_out += real_in[k] * vec_real - imag_in[k] * vec_imag
                            imag_out += real_in[k] * vec_imag + imag_in[k] * vec_real
                        turned[turned_at(step, index, side, piece_at % 2), mode] = jnp.concatenate(
                            [real_out, imag_out], axis=0
                        ).astype(jnp.bfloat16)
                    send_last(step, index, gather, side, piece_at % 2)

    gather_step(steps[0])
    send_first(steps[2])
    eigvec_all().wait_recv()
    for turn in range(len(near)):
        flat = all_eigvec[turn]
        for entry in range(entries):
            vectors[turn, entry] = jnp.broadcast_to(flat[:, entry : entry + 1], (q_local, lanes))
    gather_step(steps[1])
    send_first(steps[3])

    @pl.when(plane < planes - 1)
    def _():
        pl.semaphore_wait(above_sem, planes - 1 - plane)

    rotate_step(steps[0])
    gather_step(steps[2])
    rotate_step(steps[1])
    gather_step(steps[3])
    rotate_step(steps[2])
    rotate_step(steps[3])

    lattice_all().wait_send()
    eigvec_all().wait_send()
    everything = gathered.at[:, :, pl.ds(0, (group - 1) * local_rp)]
    bundle(everything, first_send.at[0], first_recv.at[0, 0]).wait_send()
    bundle(leaving, middle_send.at[0], middle_recv.at[0, 0, 0]).wait_send()
    for index, gather, _ in sets:
        last_own(index, gather, me // gather % 2).wait()
    last_all().wait_recv()
    last_all().wait_send()


def spread_kernel(planes, held, out, rows_of, sems):
    _, modes, tile, lanes = held.shape
    blocks = held.shape[0] // planes
    q_local = tile // 2
    per_plane = modes * blocks * 2
    per_q = rows_of.shape[0] // q_local
    by_q = rows_of.reshape(q_local, per_q, lanes)

    def spread(source):
        rows = pl.ds(source * per_plane, per_plane)
        return pltpu.make_async_copy(by_q.at[:, rows], out.at[:, rows], sems.at[source])

    for source in range(planes):
        for mode in range(modes):
            for block in range(blocks):
                values = held[source * blocks + block, mode].astype(jnp.float32)
                row = source * per_plane + (mode * blocks + block) * 2
                rows_of[pl.ds(row, q_local, stride=per_q), :] = values[:q_local]
                rows_of[pl.ds(row + 1, q_local, stride=per_q), :] = values[q_local:]
        spread(source).start()
    for source in range(planes):
        spread(source).wait()


def in_hbm(value):
    return pltpu.with_memory_space_constraint(value, pltpu.HBM)


def exchanged(coupling, rp_coords, degeneracy, qpoints, eigvec):
    n = lax.axis_size("rp")
    planes = lax.axis_size("re")
    local_rp, local_re, parts, modes, pairs = coupling.shape
    q_local = eigvec.shape[0]
    lanes = pairs // planes // n
    group = n // 2
    tile = parts * q_local
    half = group * tile
    width = group * local_rp * parts
    entries = parts * modes * modes
    near = 6
    gathered = pl.pallas_call(
        functools.partial(rotation_kernel, n, planes),
        out_shape=jax.ShapeDtypeStruct((planes * n, modes, tile, lanes), jnp.bfloat16),
        in_specs=[
            pl.BlockSpec(memory_space=pltpu.HBM),
            pl.BlockSpec(memory_space=pltpu.HBM),
            pl.BlockSpec(memory_space=pltpu.HBM),
            pl.BlockSpec(memory_space=pltpu.HBM),
            pl.BlockSpec(memory_space=pltpu.HBM),
        ],
        out_specs=pl.BlockSpec(memory_space=pl.ANY),
        scratch_shapes=[
            pltpu.VMEM(qpoints.shape, jnp.int32),
            pltpu.VMEM((planes, 2, group * local_rp, modes, parts, lanes), jnp.bfloat16),
            pltpu.VMEM((local_rp, modes, parts, pairs // planes), jnp.bfloat16),
            pltpu.VMEM((2, group, rp_coords.shape[0] + 1, local_rp), jnp.int32),
            pltpu.VMEM((modes * modes, parts, q_local), jnp.float32),
            pltpu.VMEM((near, q_local, lanes), jnp.float32),
            pltpu.VMEM((2, 2 * half, width), jnp.float32),
            pltpu.VMEM((near, entries, q_local, lanes), jnp.float32),
            pltpu.VMEM((planes, 2, half, modes * lanes), jnp.float32),
            pltpu.VMEM((planes, 2, half, modes * lanes), jnp.bfloat16),
            pltpu.VMEM((planes, 2, half, modes * lanes), jnp.bfloat16),
            pltpu.VMEM((planes * n, modes, tile, lanes), jnp.bfloat16),
            pltpu.SemaphoreType.DMA((17,)),
            pltpu.SemaphoreType.DMA((2,)),
            pltpu.SemaphoreType.DMA((2,)),
            pltpu.SemaphoreType.DMA((1,)),
            pltpu.SemaphoreType.DMA((planes, 2)),
            pltpu.SemaphoreType.DMA((1,)),
            pltpu.SemaphoreType.DMA((planes, 2, 4)),
            pltpu.SemaphoreType.DMA((1,)),
            pltpu.SemaphoreType.DMA((1,)),
            pltpu.SemaphoreType.REGULAR,
        ],
        compiler_params=pltpu.CompilerParams(
            collective_id=0, has_side_effects=True, vmem_limit_bytes=24 * 2**20
        ),
    )(
        in_hbm(jnp.swapaxes(coupling[:, 0], 1, 2)),
        in_hbm(rp_coords),
        in_hbm(degeneracy[None, :]),
        in_hbm(jnp.transpose(eigvec, (2, 3, 1, 0)).reshape(modes * modes, parts, q_local)),
        in_hbm(qpoints),
    )
    rows = planes * modes * n * parts
    spread = pl.pallas_call(
        functools.partial(spread_kernel, planes),
        out_shape=jax.ShapeDtypeStruct((q_local, rows, lanes), jnp.float32),
        in_specs=[pl.BlockSpec(memory_space=pltpu.VMEM)],
        out_specs=pl.BlockSpec(memory_space=pl.ANY),
        scratch_shapes=[
            pltpu.VMEM((q_local * (rows + 8), lanes), jnp.float32),
            pltpu.SemaphoreType.DMA((planes,)),
        ],
        compiler_params=pltpu.CompilerParams(vmem_limit_bytes=24 * 2**20),
    )(gathered)
    spread = spread.reshape(q_local, planes, modes, n, parts, lanes)
    spread = jnp.transpose(spread, (0, 1, 4, 2, 3, 5))
    return spread.reshape(q_local, planes, parts, modes, n * lanes)


def fits(n, planes, coupling, eigvec):
    local_rp, local_re, parts, modes, pairs = coupling.shape
    return (
        local_re == 1
        and n == 8
        and planes == 4
        and local_rp * n == 128
        and parts * modes * modes <= 128
        and pairs // planes // n == 128
        and eigvec.shape[0] == 8
        and modes <= 8
    )


def either(coupling, rp_coords, degeneracy, qpoints, eigvec):
    if fits(lax.axis_size("rp"), lax.axis_size("re"), coupling, eigvec):
        return exchanged(coupling, rp_coords, degeneracy, qpoints, eigvec)
    return per_device(coupling, rp_coords, degeneracy, qpoints, eigvec)


def solution(mesh):
    return jax.shard_map(
        either,
        mesh=mesh,
        in_specs=(
            P("rp", "re", None, None, None),
            P(None, "rp"),
            P("rp"),
            P(),
            P("rp", None, None, None),
        ),
        out_specs=P("rp", None, None, None, "re"),
        check_vma=False,
    )
```
